32 devices in a mesh: dp: 8 (over z, y), tensor: 4 (over x, core).
Axes of the slice: x: 2, y: 2, z: 4, core: 2. Of those that a mesh axis runs over, the one named last changes fastest.
Arguments:
- tokens: bfloat16 [37632, 768], P(('dp', 'tensor')), may hold values from -21 to 21
- res_class: int32 [192], P('dp'), may hold values from 0 to 1
- gain_attn: float32 [768], replicated, may hold values from 0.5 to 1.5
- shift_attn: float32 [768], replicated, may hold values from -1.5 to 1.5
- w_qkv: bfloat16 [768, 3, 768], P(None, None, 'tensor'), may hold values from -0.3125 to 0.3125
- bias_qv: float32 [2, 768], P(None, 'tensor'), may hold values from -1.5 to 1.5
- w_out: bfloat16 [768, 768], P('tensor'), may hold values from -0.625 to 0.625
- bias_out: float32 [768], replicated, may hold values from -1.5 to 1.5
- gain_mlp: float32 [768], replicated, may hold values from 0.5 to 1.5
- shift_mlp: float32 [768], replicated, may hold values from -1.5 to 1.5
- w_up: bfloat16 [768, 3072], P(None, 'tensor'), may hold values from -0.21875 to 0.21875
- bias_up: float32 [3072], P('tensor'), may hold values from -1.5 to 1.5
- w_down: bfloat16 [3072, 768], P('tensor'), may hold values from -0.15625 to 0.15625
- bias_down: float32 [768], replicated, may hold values from -1.5 to 1.5
- cotangent: bfloat16 [37632, 768], P(('dp', 'tensor')), may hold values from -21 to 21
Outputs:
- block_out: bfloat16 [37632, 768], P(('dp', 'tensor'))
- grad_tokens: float32 [37632, 768], P(('dp', 'tensor'))
- grad_gain_attn: float32 [768], replicated
- grad_shift_attn: float32 [768], replicated
- grad_qkv: float32 [768, 3, 768], P(None, None, 'tensor')
- grad_bias_qv: float32 [2, 768], P(None, 'tensor')
- grad_out: float32 [768, 768], P('tensor')
- grad_bias_out: float32 [768], replicated
- grad_gain_mlp: float32 [768], replicated
- grad_shift_mlp: float32 [768], replicated
- grad_up: float32 [768, 3072], P(None, 'tensor')
- grad_bias_up: float32 [3072], P('tensor')
- grad_down: float32 [3072, 768], P('tensor')
- grad_bias_down: float32 [768], replicated
- rms: float32 [3], replicated
The draws below stay inside these ranges and needn't reach their ends.
All inputs are finite; a program needn't handle non-finite values.
Results may differ from the reference program's by a relative error of at most 0.017.
Values may be sent and summed in bfloat16 or wider, within the bound.
A program may use at most 256 MiB of HBM per device.

```python
import jax
import jax.numpy as jnp
from jax import lax

D = 768
HEADS = 12
HEAD_DIM = 64
FF = 3072
PATCHES = 196
PATCHES_LOW = 144
IMG_DEV = 24
IMAGES = 192
TOKENS = 37632


def rising_rows(key, salt):
    base = jax.random.fold_in(key, salt)
    first = jax.random.fold_in(base, 0)
    image = jnp.arange(TOKENS) // PATCHES
    frac = (image.astype(jnp.float32) / max(IMAGES - 1, 1))[:, None]
    noise = jnp.clip(jax.random.normal(first, (TOKENS, D), jnp.float32), -4.0, 4.0)
    values = noise * (0.6 + 1.2 * frac)
    return values.astype(jnp.bfloat16)


def draw_tokens(key, part):
    return rising_rows(key, 11)


def draw_cotangent(key, part):
    return rising_rows(key, 23)


def touch_ends(array, rng, low, top_value):
    longest = array.shape.index(max(array.shape))
    spots = []
    for shift in (0, 1):
        where = [jax.random.randint(jax.random.fold_in(rng, axis), (), 0, length) for axis, length in enumerate(array.shape)]
        where[longest] = (where[longest] + shift) % array.shape[longest]
        spots.append(tuple(where))
    return array.at[spots[0]].set(low).at[spots[1]].set(top_value)


def block_levels(own_key, dims, shards, smallest, largest):
    loudness = 1.0
    for axis_at, blocks in shards:
        steps = jax.random.uniform(jax.random.fold_in(jax.random.fold_in(own_key, 6), axis_at), (blocks,), jnp.float32, smallest / len(shards), largest / len(shards))
        loudness = loudness * jnp.repeat(jnp.exp(steps), dims[axis_at] // blocks).reshape((-1,) + (1,) * (len(dims) - 1 - axis_at))
    return loudness


def bell_draw(rng, extent, deviation, limit, pieces=(), kind=jnp.bfloat16):
    result = jax.random.normal(rng, extent, jnp.float32) * deviation
    if len(pieces) > 0:
        result = block_levels(rng, extent, pieces, -0.22, 0.18) * result
    return jnp.clip(result, min=-limit, max=limit).astype(kind)


def setup_inputs(seed: int = 0) -> dict:
    splits = jax.random.split(jax.random.key(seed), 16)
    return {
        "tokens": draw_tokens(jax.random.fold_in(splits[15], 71), 0),
        "res_class": touch_ends(jax.random.randint(splits[1], (IMAGES,), 0, 2), jax.random.fold_in(splits[1], 1), 0, 1).astype(jnp.int32),
        "gain_attn": jnp.clip(1.0 + 0.1 * jax.random.normal(splits[2], (D,), jnp.float32), 0.5, 1.5),
        "shift_attn": bell_draw(splits[3], (D,), 0.3, 1.5, (), jnp.float32),
        "w_qkv": bell_draw(splits[4], (D, 3, D), (D // 2) ** -0.5, 0.3125, ((2, 4),)),
        "bias_qv": bell_draw(splits[5], (2, D), 0.3, 1.5, ((1, 4),), jnp.float32),
        "w_out": bell_draw(splits[6], (D, D), (D // 8) ** -0.5, 0.625, ((0, 4),)),
        "bias_out": bell_draw(splits[7], (D,), 0.3, 1.5, (), jnp.float32),
        "gain_mlp": jnp.clip(1.0 + 0.1 * jax.random.normal(splits[8], (D,), jnp.float32), 0.5, 1.5),
        "shift_mlp": bell_draw(splits[9], (D,), 0.3, 1.5, (), jnp.float32),
        "w_up": bell_draw(splits[10], (D, FF), D ** -0.5, 0.21875, ((1, 4),)),
        "bias_up": bell_draw(splits[11], (FF,), 0.3, 1.5, ((0, 4),), jnp.float32),
        "w_down": bell_draw(splits[12], (FF, D), (FF // 2) ** -0.5, 0.15625, ((0, 4),)),
        "bias_down": bell_draw(splits[13], (D,), 0.3, 1.5, (), jnp.float32),
        "cotangent": draw_cotangent(jax.random.fold_in(splits[15], 71), 0),
    }


@jax.custom_vjp
def low(v):
    return lax.optimization_barrier(v.astype(jnp.bfloat16)).astype(jnp.float32)

@jax.custom_vjp
def low_back(v):
    return v

def low_keep(v):
    return (low(v), None)

def low_pass(kept, grad):
    return (grad,)

def back_keep(v):
    return (v, None)

def back_low(kept, grad):
    return (low(grad),)
low.defvjp(low_keep, low_pass)
low_back.defvjp(back_keep, back_low)
EPS = 1e-06

def highest(left, right):
    return jnp.dot(left, right, precision=lax.Precision.HIGHEST)

def layer_norm(values, gain, shift):
    mean = lax.optimization_barrier(jnp.mean(values, axis=-1, keepdims=True))
    centred = values - mean
    variance = lax.optimization_barrier(jnp.mean(centred * centred, axis=-1, keepdims=True))
    return centred * lax.rsqrt(variance + EPS) * gain + shift

def attend_block(query, key, value, valid):
    scale = HEAD_DIM ** (-0.5)
    scores = jnp.einsum('iqhd,ikhd->ihqk', query, key, precision=lax.Precision.HIGHEST)
    scores = low_back(scale * scores)
    scores = jnp.where(valid[:, None, None, :], scores, -1e+30)
    total = jax.nn.logsumexp(scores, axis=-1, keepdims=True)
    probs = low(jnp.exp(scores - total))
    return jnp.einsum('ihqk,ikhd->iqhd', probs, value, precision=lax.Precision.HIGHEST)

def reference(tokens, res_class, gain_attn, shift_attn, w_qkv, bias_qv, w_out, bias_out, gain_mlp, shift_mlp, w_up, bias_up, w_down, bias_down, cotangent):
    counts = jnp.where(res_class == 0, PATCHES, PATCHES_LOW)
    key_valid = jnp.arange(PATCHES)[None, :] < counts[:, None]
    row_valid = key_valid.reshape(-1).astype(jnp.float32)[:, None]
    groups = IMAGES // IMG_DEV
    shape = (groups, IMG_DEV, PATCHES, HEADS, HEAD_DIM)
    valid_blocks = key_valid.reshape(groups, IMG_DEV, PATCHES)
    block_fn = jax.checkpoint(attend_block)

    def forward(xf, g1, s1, wqkv, bqv, wout, bout, g2, s2, wup, bup, wdown, bdown):
        n1 = low(layer_norm(xf, g1, s1))
        qkv = highest(n1, wqkv.reshape(D, 3 * D)).reshape(-1, 3, D)
        query = low(low_back(qkv[:, 0] + bqv[0]))
        key = low(low_back(qkv[:, 1]))
        value = low(low_back(qkv[:, 2] + bqv[1]))
        context = lax.map(lambda blk: block_fn(*blk), (query.reshape(shape), key.reshape(shape), value.reshape(shape), valid_blocks))
        context = low(low_back(context.reshape(-1, D)))
        branch = low_back(highest(context, wout)) + bout
        hidden = xf + branch
        n2 = low(layer_norm(hidden, g2, s2))
        pre_act = low_back(highest(n2, wup)) + bup
        act = low(jax.nn.gelu(pre_act, approximate=False))
        mlp = low_back(highest(act, wdown)) + bdown
        return ((hidden + mlp) * row_valid, (branch, mlp))
    primals = (tokens.astype(jnp.float32), gain_attn, shift_attn, w_qkv.astype(jnp.float32), bias_qv, w_out.astype(jnp.float32), bias_out, gain_mlp, shift_mlp, w_up.astype(jnp.float32), bias_up, w_down.astype(jnp.float32), bias_down)
    stream, pullback, aux = jax.vjp(forward, *primals, has_aux=True)
    branch, mlp = aux
    grads = pullback(cotangent.astype(jnp.float32))
    total = jnp.sum(row_valid) * D
    sums = jnp.stack([jnp.sum(stream * stream), jnp.sum(branch * branch * row_valid), jnp.sum(mlp * mlp * row_valid)])
    rms = jnp.sqrt(sums / total)
    return (stream.astype(jnp.bfloat16), grads[0], grads[1], grads[2], grads[3], grads[4], grads[5], grads[6], grads[7], grads[8], grads[9], grads[10], grads[11], grads[12], rms)
```

```python
import jax
import jax.numpy as jnp
from jax import lax
from jax.sharding import PartitionSpec as P

HEAD_DIM = 64
PATCHES = 196
PATCHES_LOW = 144
EPS = 1e-06
F32 = jnp.float32
BF16 = jnp.bfloat16


def normalize(values):
    mean = jnp.mean(values, axis=-1, keepdims=True)
    centred = values - mean
    factor = lax.rsqrt(jnp.mean(centred * centred, axis=-1, keepdims=True) + EPS)
    return (centred * factor, factor)


def norm_back(grad_out, gain, normed, factor):
    scaled = grad_out * gain
    return factor * (
        scaled
        - jnp.mean(scaled, axis=-1, keepdims=True)
        - normed * jnp.mean(scaled * normed, axis=-1, keepdims=True)
    )


def dot(a, b, dims):
    return lax.dot_general(a, b, (dims, ((), ())), preferred_element_type=F32)


NN = ((1,), (0,))
NT = ((1,), (1,))
TN = ((0,), (0,))


def on_device(
    tokens,
    res_class,
    gain_attn,
    shift_attn,
    w_qkv,
    bias_qv,
    w_out,
    bias_out,
    gain_mlp,
    shift_mlp,
    w_up,
    bias_up,
    w_down,
    bias_down,
    cotangent,
):
    rows, width = tokens.shape
    local = w_qkv.shape[2]
    images = rows // PATCHES
    parts = lax.axis_size("tensor")
    heads_here = local // HEAD_DIM
    heads = parts * heads_here
    scale = HEAD_DIM ** (-0.5)
    place = lax.axis_index("tensor")
    ff_local = w_up.shape[1]

    gather = lambda v: lax.all_gather(v, "tensor", axis=0, tiled=False)
    full_qkv = gather(w_qkv.reshape(width, 3 * local))
    full_out = gather(w_out)
    full_up = gather(w_up)
    full_down = gather(w_down)
    bias_q_full = gather(jnp.concatenate([bias_qv[0], bias_qv[1], bias_up]))
    bq = bias_q_full[:, :local]
    bv = bias_q_full[:, local : 2 * local]
    bu = bias_q_full[:, 2 * local :]

    classes = lax.dynamic_slice_in_dim(res_class, place * images, images)
    counts = jnp.where(classes == 0, PATCHES, PATCHES_LOW)
    key_valid = jnp.arange(PATCHES)[None, :] < counts[:, None]
    row_valid = key_valid.reshape(-1).astype(F32)[:, None]
    mask = key_valid[:, None, None, :]

    inputs = tokens.astype(F32)
    normed_a, factor_a = normalize(inputs)
    in_attn = (normed_a * gain_attn + shift_attn).astype(BF16)
    shape = (images, PATCHES, heads_here, HEAD_DIM)
    saved = []
    context = []
    for s in range(parts):
        qkv = dot(in_attn, full_qkv[s], NN)
        query = (qkv[:, :local] + bq[s]).astype(BF16).reshape(shape)
        keys = qkv[:, local : 2 * local].astype(BF16).reshape(shape)
        values = (qkv[:, 2 * local :] + bv[s]).astype(BF16).reshape(shape)
        scores = jnp.einsum("iqhd,ikhd->ihqk", query, keys, preferred_element_type=F32) * scale
        scores = jnp.where(mask, scores, -1e30)
        log_total = jax.nn.logsumexp(scores, axis=-1, keepdims=True)
        probs = jnp.exp(scores - log_total).astype(BF16)
        part = jnp.einsum("ihqk,ikhd->iqhd", probs, values, preferred_element_type=F32)
        context.append(part.reshape(-1, local).astype(BF16))
        saved.append((query, keys, values, probs))
    branch = sum(dot(context[s], full_out[s], NN) for s in range(parts)) + bias_out
    hidden = inputs + branch
    normed_m, factor_m = normalize(hidden)
    in_mlp = (normed_m * gain_mlp + shift_mlp).astype(BF16)
    acts = []
    slopes = []
    mlp = bias_down
    for s in range(parts):
        pre = dot(in_mlp, full_up[s], NN) + bu[s]
        cdf = 0.5 * (1.0 + lax.erf(pre * (2.0 ** -0.5)))
        acts.append((pre * cdf).astype(BF16))
        slopes.append((cdf + pre * jnp.exp(-0.5 * pre * pre) * 0.3989422804014327).astype(BF16))
        mlp = mlp + dot(acts[s], full_down[s], NN)
    stream = (hidden + mlp) * row_valid
    block_out = stream.astype(BF16)

    grad_stream = cotangent.astype(F32) * row_valid
    grad_low = grad_stream.astype(BF16)
    grad_bias_down = jnp.sum(grad_stream, axis=0)
    weight_down, weight_up, grad_bias_up = [], [], []
    grad_in_mlp = 0.0
    for s in range(parts):
        grad_pre = dot(grad_low, full_down[s], NT) * slopes[s].astype(F32)
        grad_bias_up.append(jnp.sum(grad_pre, axis=0))
        grad_pre_low = grad_pre.astype(BF16)
        weight_down.append(dot(acts[s], grad_low, TN).astype(BF16))
        weight_up.append(dot(in_mlp, grad_pre_low, TN).astype(BF16))
        grad_in_mlp = grad_in_mlp + dot(grad_pre_low, full_up[s], NT)
    grad_gain_mlp = jnp.sum(grad_in_mlp * normed_m, axis=0)
    grad_shift_mlp = jnp.sum(grad_in_mlp, axis=0)
    grad_hidden = grad_stream + norm_back(grad_in_mlp, gain_mlp, normed_m, factor_m)
    grad_bias_out = jnp.sum(grad_hidden, axis=0)
    grad_branch = grad_hidden.astype(BF16)

    scatter = lambda v: lax.psum_scatter(v, "tensor", scatter_dimension=0, tiled=False)
    w_mlp = scatter(jnp.stack([jnp.concatenate([u, d], 0) for u, d in zip(weight_up, weight_down)]))
    w_mlp = lax.psum(w_mlp, "dp")

    weight_out, weight_qkv, bias_grads = [], [], []
    grad_in_attn = 0.0
    for s in range(parts):
        query, keys, values, probs = saved[s]
        weight_out.append(dot(context[s], grad_branch, TN).astype(BF16))
        grad_context = dot(grad_branch, full_out[s], NT).astype(BF16).reshape(shape)
        grad_value = jnp.einsum(
            "ihqk,iqhd->ikhd", probs, grad_context, preferred_element_type=F32
        )
        grad_probs = jnp.einsum(
            "iqhd,ikhd->ihqk", grad_context, values, preferred_element_type=F32
        )
        probs_full = probs.astype(F32)
        row_dot = jnp.sum(probs_full * grad_probs, axis=-1, keepdims=True)
        grad_scores = (probs_full * (grad_probs - row_dot)).astype(BF16)
        grad_query = scale * jnp.einsum(
            "ihqk,ikhd->iqhd", grad_scores, keys, preferred_element_type=F32
        )
        grad_key = scale * jnp.einsum(
            "ihqk,iqhd->ikhd", grad_scores, query, preferred_element_type=F32
        )
        low = jnp.concatenate(
            [g.reshape(-1, local).astype(BF16) for g in (grad_query, grad_key, grad_value)], axis=1
        )
        bias_grads.append(jnp.sum(low.astype(F32), axis=0))
        weight_qkv.append(dot(in_attn, low, TN).astype(BF16))
        grad_in_attn = grad_in_attn + dot(low, full_qkv[s], NT)
    w_out_g = scatter(jnp.stack(weight_out))
    w_qkv_g = scatter(jnp.stack(weight_qkv))
    w_out_g, w_qkv_g = lax.psum((w_out_g, w_qkv_g), "dp")
    grad_gain_attn = jnp.sum(grad_in_attn * normed_a, axis=0)
    grad_shift_attn = jnp.sum(grad_in_attn, axis=0)
    grad_tokens = grad_hidden + norm_back(grad_in_attn, gain_attn, normed_a, factor_a)
    totals = jnp.stack(
        [
            jnp.sum(stream * stream),
            jnp.sum(branch * branch * row_valid),
            jnp.sum(mlp * mlp * row_valid),
            jnp.sum(row_valid),
        ]
    )
    pieces = [
        grad_gain_attn,
        grad_shift_attn,
        grad_bias_out,
        grad_gain_mlp,
        grad_shift_mlp,
        grad_bias_down,
        jnp.stack([b[:local] for b in bias_grads]).reshape(-1),
        jnp.stack([b[2 * local :] for b in bias_grads]).reshape(-1),
        jnp.concatenate(grad_bias_up),
        totals,
    ]
    summed = lax.psum(jnp.concatenate(pieces), ("dp", "tensor"))
    got = []
    at = 0
    for p in pieces:
        got.append(summed[at : at + p.shape[0]])
        at += p.shape[0]
    mine = lambda v, n: lax.dynamic_slice_in_dim(v, place * n, n)
    sums = got[9]
    rms = jnp.sqrt(sums[:3] / (sums[3] * width))
    return (
        block_out,
        grad_tokens,
        got[0],
        got[1],
        w_qkv_g.astype(F32).reshape(width, 3, local),
        jnp.stack([mine(got[6], local), mine(got[7], local)]),
        w_out_g.astype(F32),
        got[2],
        got[3],
        got[4],
        w_mlp[:width].astype(F32),
        mine(got[8], ff_local),
        w_mlp[width:].astype(F32),
        got[5],
        rms,
    )


def solution(mesh):
    row = P(("dp", "tensor"), None)
    in_specs = (
        row, P("dp"), P(), P(), P(None, None, "tensor"), P(None, "tensor"), P("tensor", None),
        P(), P(), P(), P(None, "tensor"), P("tensor"), P("tensor", None), P(), row,
    )
    out_specs = (
        row, row, P(), P(), P(None, None, "tensor"), P(None, "tensor"), P("tensor", None),
        P(), P(), P(), P(None, "tensor"), P("tensor"), P("tensor", None), P(), P(),
    )
    return jax.shard_map(
        on_device, mesh=mesh, in_specs=in_specs, out_specs=out_specs, check_vma=False
    )
```

```python
import functools

import jax
import jax.numpy as jnp
from jax import lax
from jax.experimental import pallas as pl
from jax.experimental.pallas import tpu as pltpu
from jax.sharding import PartitionSpec as P

HEAD_DIM = 64
PATCHES = 196
PATCHES_LOW = 144
PADDED = 208
LANES = 128
EPS = 1e-06
F32 = jnp.float32
BF16 = jnp.bfloat16


def normalize(values):
    mean = jnp.mean(values, axis=-1, keepdims=True)
    centred = values - mean
    factor = lax.rsqrt(jnp.mean(centred * centred, axis=-1, keepdims=True) + EPS)
    return (centred * factor, factor)


def norm_back(grad_out, gain, normed, factor):
    scaled = grad_out * gain
    return factor * (
        scaled
        - jnp.mean(scaled, axis=-1, keepdims=True)
        - normed * jnp.mean(scaled * normed, axis=-1, keepdims=True)
    )


def dot(a, b, dims):
    return lax.dot_general(a, b, (dims, ((), ())), preferred_element_type=F32)


NN = ((1,), (0,))
NT = ((1,), (1,))
TN = ((0,), (0,))


def head_masks(factor):
    lane = lax.broadcasted_iota(jnp.int32, (1, LANES), 1)
    first = jnp.where(lane < HEAD_DIM, factor, 0.0)
    return first.astype(BF16), (factor - first).astype(BF16)


def attend_kernel(group, counts, qkv, context, probs):
    rows = qkv.shape[0]
    valid = counts[pl.program_id(0)]
    keep = lax.broadcasted_iota(jnp.int32, (rows, rows), 1) < valid
    ones = head_masks(1.0)
    scaled = head_masks(HEAD_DIM ** (-0.5))
    for j in range(group // LANES):
        at = j * LANES
        query = qkv[:, at : at + LANES]
        key = qkv[:, group + at : group + at + LANES]
        value = qkv[:, 2 * group + at : 2 * group + at + LANES]
        total = None
        for h in range(2):
            scores = dot(query * scaled[h], key, NT)
            scores = jnp.where(keep, scores, -1e30)
            top = jnp.max(scores, axis=-1, keepdims=True)
            raised = jnp.exp(scores - top)
            low = (raised * (1.0 / jnp.sum(raised, axis=-1, keepdims=True))).astype(BF16)
            probs[0, 2 * j + h] = low
            part = dot(low, value * ones[h], NN)
            total = part if total is None else total + part
        context[:, at : at + LANES] = total.astype(BF16)


def attend_back_kernel(group, qkv, probs, grad_context, grads):
    ones = head_masks(1.0)
    scaled = head_masks(HEAD_DIM ** (-0.5))
    for j in range(group // LANES):
        at = j * LANES
        query = qkv[:, at : at + LANES]
        key = qkv[:, group + at : group + at + LANES]
        value = qkv[:, 2 * group + at : 2 * group + at + LANES]
        grad = grad_context[:, at : at + LANES]
        sums = None
        for h in range(2):
            own = grad * ones[h]
            low = probs[0, 2 * j + h]
            wide = low.astype(F32)
            grad_probs = dot(own, value, NT)
            row_dot = jnp.sum(wide * grad_probs, axis=-1, keepdims=True)
            grad_scores = (wide * (grad_probs - row_dot)).astype(BF16)
            parts = (
                dot(grad_scores, key * scaled[h], NN),
                dot(grad_scores, query * scaled[h], TN),
                dot(low, own, TN),
            )
            sums = parts if sums is None else [a + b for a, b in zip(sums, parts)]
        for i in range(3):
            grads[:, i * group + at : i * group + at + LANES] = sums[i].astype(BF16)


def attend(counts, qkv):
    images = counts.shape[0]
    rows = qkv.shape[0] // images
    group = qkv.shape[1] // 3
    heads = group // HEAD_DIM
    return pl.pallas_call(
        functools.partial(attend_kernel, group),
        grid_spec=pltpu.PrefetchScalarGridSpec(
            num_scalar_prefetch=1,
            grid=(images,),
            in_specs=[pl.BlockSpec((rows, 3 * group), lambda i, c: (i, 0))],
            out_specs=[
                pl.BlockSpec((rows, group), lambda i, c: (i, 0)),
                pl.BlockSpec((1, heads, rows, rows), lambda i, c: (i, 0, 0, 0)),
            ],
        ),
        out_shape=[
            jax.ShapeDtypeStruct((images * rows, group), BF16),
            jax.ShapeDtypeStruct((images, heads, rows, rows), BF16),
        ],
        cost_estimate=pl.CostEstimate(
            flops=images * heads * rows * rows * HEAD_DIM * 16,
            bytes_accessed=images * rows * group * 8,
            transcendentals=images * heads * rows * rows,
        ),
        name="attend",
    )(counts, qkv)


def attend_back(qkv, probs, grad_context):
    images, heads, rows, _ = probs.shape
    group = qkv.shape[1] // 3
    wide = pl.BlockSpec((rows, 3 * group), lambda i: (i, 0))
    return pl.pallas_call(
        functools.partial(attend_back_kernel, group),
        grid=(images,),
        in_specs=[
            wide,
            pl.BlockSpec((1, heads, rows, rows), lambda i: (i, 0, 0, 0)),
            pl.BlockSpec((rows, group), lambda i: (i, 0)),
        ],
        out_specs=wide,
        out_shape=jax.ShapeDtypeStruct(qkv.shape, BF16),
        cost_estimate=pl.CostEstimate(
            flops=images * heads * rows * rows * HEAD_DIM * 40,
            bytes_accessed=images * rows * group * 16,
            transcendentals=0,
        ),
        name="attend_back",
    )(qkv, probs, grad_context)


def swap(value, axis, bit):
    size = lax.axis_size(axis)
    return lax.ppermute(value, axis, [(i, i ^ bit) for i in range(size)])


def after(value, *earlier):
    return lax.optimization_barrier((value, *earlier))[0]


def on_device(
    tokens,
    res_class,
    gain_attn,
    shift_attn,
    w_qkv,
    bias_qv,
    w_out,
    bias_out,
    gain_mlp,
    shift_mlp,
    w_up,
    bias_up,
    w_down,
    bias_down,
    cotangent,
):
    rows, width = tokens.shape
    local = w_qkv.shape[2]
    images = rows // PATCHES
    place = lax.axis_index("tensor")
    ff_local = w_up.shape[1]
    group = 2 * local

    def gather(value, *earlier):
        value = after(value, *earlier) if earlier else value
        far = swap(value, "tensor", 2)
        return [value, swap(value, "tensor", 1), far, swap(far, "tensor", 1)]

    biases = gather(jnp.concatenate([bias_qv.reshape(-1), bias_up]))
    qkv_w = gather(w_qkv)
    out_w = gather(w_out, qkv_w[2])
    up_w = gather(w_up, out_w[2])
    down_w = gather(w_down, up_w[2])
    bq = [b[:local] for b in biases]
    bv = [b[local : 2 * local] for b in biases]
    bu = [b[2 * local :] for b in biases]

    def pad(value):
        split = value.reshape(images, PATCHES, -1)
        return jnp.pad(split, ((0, 0), (0, PADDED - PATCHES), (0, 0))).reshape(images * PADDED, -1)

    def unpad(value):
        return value.reshape(images, PADDED, -1)[:, :PATCHES].reshape(rows, -1)

    classes = lax.dynamic_slice_in_dim(res_class, place * images, images)
    counts = jnp.where(classes == 0, PATCHES, PATCHES_LOW)
    key_valid = jnp.arange(PADDED)[None, :] < counts[:, None]
    row_valid = key_valid.reshape(-1).astype(F32)[:, None]

    inputs = pad(tokens).astype(F32)
    normed_a, factor_a = normalize(inputs)
    in_attn = (normed_a * gain_attn + shift_attn).astype(BF16)

    zero = jnp.zeros((group,), F32)
    saved = []
    branch = bias_out
    for g in range(2):
        pair = (2 * g, 2 * g + 1)
        w_pair = jnp.stack([qkv_w[r] for r in pair], axis=2).reshape(width, 3 * group)
        out_pair = jnp.concatenate([out_w[r] for r in pair], axis=0)
        bias = jnp.concatenate([bq[pair[0]], bq[pair[1]], zero, bv[pair[0]], bv[pair[1]]])
        qkv = (dot(in_attn, w_pair, NN) + bias).astype(BF16)
        context, probs = attend(counts, qkv)
        branch = branch + dot(context, out_pair, NN)
        saved.append((w_pair, out_pair, qkv, context, probs))
    hidden = inputs + branch
    normed_m, factor_m = normalize(hidden)
    in_mlp = (normed_m * gain_mlp + shift_mlp).astype(BF16)
    acts = []
    slopes = []
    mlp = bias_down
    for r in range(4):
        pre = dot(in_mlp, up_w[r], NN) + bu[r]
        cdf = 0.5 * (1.0 + lax.erf(pre * (2.0 ** -0.5)))
        acts.append((pre * cdf).astype(BF16))
        slopes.append((cdf + pre * jnp.exp(-0.5 * pre * pre) * 0.3989422804014327).astype(BF16))
        mlp = mlp + dot(acts[r], down_w[r], NN)
    stream = (hidden + mlp) * row_valid
    block_out = unpad(stream.astype(BF16))

    def scatter(parts):
        near = parts[0] + swap(parts[1], "tensor", 1)
        far = parts[2] + swap(parts[3], "tensor", 1)
        return near + swap(far, "tensor", 2)

    grad_stream = pad(cotangent).astype(F32) * row_valid
    grad_low = grad_stream.astype(BF16)
    grad_bias_down = jnp.sum(grad_stream, axis=0)
    d_down = [dot(acts[r], grad_low, TN).astype(BF16) for r in range(4)]
    d_up, d_bias_up = [], []
    grad_in_mlp = 0.0
    for r in range(4):
        grad_pre = dot(grad_low, down_w[r], NT) * slopes[r].astype(F32)
        d_bias_up.append(jnp.sum(grad_pre, axis=0))
        grad_pre_low = grad_pre.astype(BF16)
        d_up.append(dot(in_mlp, grad_pre_low, TN).astype(BF16))
        grad_in_mlp = grad_in_mlp + dot(grad_pre_low, up_w[r], NT)
    own_down = lax.psum(scatter(d_down), "dp")
    own_up = lax.psum(after(scatter(d_up), own_down), "dp")

    grad_gain_mlp = jnp.sum(grad_in_mlp * normed_m, axis=0)
    grad_shift_mlp = jnp.sum(grad_in_mlp, axis=0)
    grad_hidden = grad_stream + norm_back(grad_in_mlp, gain_mlp, normed_m, factor_m)
    grad_bias_out = jnp.sum(grad_hidden, axis=0)
    grad_branch = after(grad_hidden.astype(BF16), *d_down, *d_up)

    d_out, d_qkv, d_bias_qv = [None] * 4, [None] * 4, [None] * 4
    grad_in_attn = 0.0
    for g in (1, 0):
        w_pair, out_pair, qkv, context, probs = saved[g]
        out_grad = dot(context, grad_branch, TN).astype(BF16)
        grad_context = dot(grad_branch, out_pair, NT).astype(BF16)
        low = attend_back(qkv, probs, grad_context)
        bias_sum = jnp.sum(low.astype(F32), axis=0).reshape(3, 2, local)
        qkv_grad = dot(in_attn, low, TN).astype(BF16).reshape(width, 3, 2, local)
        for k in range(2):
            r = 2 * g + k
            d_out[r] = out_grad[k * local : (k + 1) * local]
            d_qkv[r] = qkv_grad[:, :, k]
            d_bias_qv[r] = jnp.concatenate([bias_sum[0, k], bias_sum[2, k]])
        grad_in_attn = grad_in_attn + dot(low, w_pair, NT)
    own_out, own_qkv = lax.psum((after(scatter(d_out), own_up), scatter(d_qkv)), "dp")
    grad_gain_attn = jnp.sum(grad_in_attn * normed_a, axis=0)
    grad_shift_attn = jnp.sum(grad_in_attn, axis=0)
    grad_tokens = unpad(grad_hidden + norm_back(grad_in_attn, gain_attn, normed_a, factor_a))
    totals = jnp.stack(
        [
            jnp.sum(stream * stream),
            jnp.sum(branch * branch * row_valid),
            jnp.sum(mlp * mlp * row_valid),
            jnp.sum(row_valid),
        ]
    )
    shared = jnp.concatenate(
        [
            grad_gain_attn,
            grad_shift_attn,
            grad_bias_out,
            grad_gain_mlp,
            grad_shift_mlp,
            grad_bias_down,
            totals,
        ]
    )
    shared = shared + swap(shared, "tensor", 1)
    shared = shared + swap(shared, "tensor", 2)
    biases = scatter([jnp.concatenate([d_bias_qv[r], d_bias_up[r]]) for r in range(4)])
    small = jnp.concatenate([biases, shared])
    bit = 1
    while bit < lax.axis_size("dp"):
        small = small + swap(small, "dp", bit)
        bit *= 2
    wide = 2 * local + ff_local
    got = [small[wide + i * width : wide + (i + 1) * width] for i in range(6)]
    sums = small[wide + 6 * width :]
    rms = jnp.sqrt(sums[:3] / (sums[3] * width))
    return (
        block_out,
        grad_tokens,
        got[0],
        got[1],
        own_qkv.astype(F32),
        small[: 2 * local].reshape(2, local),
        own_out.astype(F32),
        got[2],
        got[3],
        got[4],
        own_up.astype(F32),
        small[2 * local : wide],
        own_down.astype(F32),
        got[5],
        rms,
    )


def solution(mesh):
    row = P(("dp", "tensor"), None)
    in_specs = (
        row, P("dp"), P(), P(), P(None, None, "tensor"), P(None, "tensor"), P("tensor", None),
        P(), P(), P(), P(None, "tensor"), P("tensor"), P("tensor", None), P(), row,
    )
    out_specs = (
        row, row, P(), P(), P(None, None, "tensor"), P(None, "tensor"), P("tensor", None),
        P(), P(), P(), P(None, "tensor"), P("tensor"), P("tensor", None), P(), P(),
    )
    return jax.shard_map(
        on_device, mesh=mesh, in_specs=in_specs, out_specs=out_specs, check_vma=False
    )
```

```python
import functools

import jax
import jax.numpy as jnp
from jax import lax
from jax.experimental import pallas as pl
from jax.experimental.pallas import tpu as pltpu
from jax.sharding import PartitionSpec as P

HEAD_DIM = 64
PATCHES = 196
PATCHES_LOW = 144
PADDED = 208
LANES = 128
EPS = 1e-06
F32 = jnp.float32
BF16 = jnp.bfloat16


def normalize(values):
    mean = jnp.mean(values, axis=-1, keepdims=True)
    centred = values - mean
    factor = lax.rsqrt(jnp.mean(centred * centred, axis=-1, keepdims=True) + EPS)
    return (centred * factor, factor)


def norm_back(grad_out, gain, normed, factor):
    scaled = grad_out * gain
    return factor * (
        scaled
        - jnp.mean(scaled, axis=-1, keepdims=True)
        - normed * jnp.mean(scaled * normed, axis=-1, keepdims=True)
    )


def dot(a, b, dims):
    return lax.dot_general(a, b, (dims, ((), ())), preferred_element_type=F32)


NN = ((1,), (0,))
NT = ((1,), (1,))
TN = ((0,), (0,))


def head_masks(factor):
    lane = lax.broadcasted_iota(jnp.int32, (1, LANES), 1)
    first = jnp.where(lane < HEAD_DIM, factor, 0.0)
    return first.astype(BF16), (factor - first).astype(BF16)


def attend_kernel(group, counts, qkv, context, probs):
    rows = qkv.shape[0]
    valid = counts[pl.program_id(0)]
    keep = lax.broadcasted_iota(jnp.int32, (rows, rows), 1) < valid
    ones = head_masks(1.0)
    scaled = head_masks(HEAD_DIM ** (-0.5))
    for j in range(group // LANES):
        at = j * LANES
        query = qkv[:, at : at + LANES]
        key = qkv[:, group + at : group + at + LANES]
        value = qkv[:, 2 * group + at : 2 * group + at + LANES]
        total = None
        for h in range(2):
            scores = dot(query * scaled[h], key, NT)
            scores = jnp.where(keep, scores, -1e30)
            top = jnp.max(scores, axis=-1, keepdims=True)
            raised = jnp.exp(scores - top)
            low = (raised * (1.0 / jnp.sum(raised, axis=-1, keepdims=True))).astype(BF16)
            probs[0, 2 * j + h] = low
            part = dot(low, value * ones[h], NN)
            total = part if total is None else total + part
        context[:, at : at + LANES] = total.astype(BF16)


def attend_back_kernel(group, qkv, probs, grad_context, grads):
    ones = head_masks(1.0)
    scaled = head_masks(HEAD_DIM ** (-0.5))
    for j in range(group // LANES):
        at = j * LANES
        query = qkv[:, at : at + LANES]
        key = qkv[:, group + at : group + at + LANES]
        value = qkv[:, 2 * group + at : 2 * group + at + LANES]
        grad = grad_context[:, at : at + LANES]
        sums = None
        for h in range(2):
            own = grad * ones[h]
            low = probs[0, 2 * j + h]
            wide = low.astype(F32)
            grad_probs = dot(own, value, NT)
            row_dot = jnp.sum(wide * grad_probs, axis=-1, keepdims=True)
            grad_scores = (wide * (grad_probs - row_dot)).astype(BF16)
            parts = (
                dot(grad_scores, key * scaled[h], NN),
                dot(grad_scores, query * scaled[h], TN),
                dot(low, own, TN),
            )
            sums = parts if sums is None else [a + b for a, b in zip(sums, parts)]
        for i in range(3):
            grads[:, i * group + at : i * group + at + LANES] = sums[i].astype(BF16)


def attend(counts, qkv):
    images = counts.shape[0]
    rows = qkv.shape[0] // images
    group = qkv.shape[1] // 3
    heads = group // HEAD_DIM
    return pl.pallas_call(
        functools.partial(attend_kernel, group),
        grid_spec=pltpu.PrefetchScalarGridSpec(
            num_scalar_prefetch=1,
            grid=(images,),
            in_specs=[pl.BlockSpec((rows, 3 * group), lambda i, c: (i, 0))],
            out_specs=[
                pl.BlockSpec((rows, group), lambda i, c: (i, 0)),
                pl.BlockSpec((1, heads, rows, rows), lambda i, c: (i, 0, 0, 0)),
            ],
        ),
        out_shape=[
            jax.ShapeDtypeStruct((images * rows, group), BF16),
            jax.ShapeDtypeStruct((images, heads, rows, rows), BF16),
        ],
        cost_estimate=pl.CostEstimate(
            flops=images * heads * rows * rows * HEAD_DIM * 16,
            bytes_accessed=images * rows * group * 8,
            transcendentals=images * heads * rows * rows,
        ),
        name="attend",
    )(counts, qkv)


def attend_back(qkv, probs, grad_context):
    images, heads, rows, _ = probs.shape
    group = qkv.shape[1] // 3
    wide = pl.BlockSpec((rows, 3 * group), lambda i: (i, 0))
    return pl.pallas_call(
        functools.partial(attend_back_kernel, group),
        grid=(images,),
        in_specs=[
            wide,
            pl.BlockSpec((1, heads, rows, rows), lambda i: (i, 0, 0, 0)),
            pl.BlockSpec((rows, group), lambda i: (i, 0)),
        ],
        out_specs=wide,
        out_shape=jax.ShapeDtypeStruct(qkv.shape, BF16),
        cost_estimate=pl.CostEstimate(
            flops=images * heads * rows * rows * HEAD_DIM * 40,
            bytes_accessed=images * rows * group * 16,
            transcendentals=0,
        ),
        name="attend_back",
    )(qkv, probs, grad_context)


def swap(value, axis, bit):
    size = lax.axis_size(axis)
    return lax.ppermute(value, axis, [(i, i ^ bit) for i in range(size)])


def after(value, *earlier):
    return lax.optimization_barrier((value, *earlier))[0]


def on_device(
    tokens,
    res_class,
    gain_attn,
    shift_attn,
    w_qkv,
    bias_qv,
    w_out,
    bias_out,
    gain_mlp,
    shift_mlp,
    w_up,
    bias_up,
    w_down,
    bias_down,
    cotangent,
):
    rows, width = tokens.shape
    local = w_qkv.shape[2]
    images = rows // PATCHES
    place = lax.axis_index("tensor")
    ff_local = w_up.shape[1]
    group = 2 * local

    def gather(value, *earlier):
        value = after(value, *earlier) if earlier else value
        far = swap(value, "tensor", 2)
        return [value, swap(value, "tensor", 1), far, swap(far, "tensor", 1)]

    biases = gather(jnp.concatenate([bias_qv.reshape(-1), bias_up]))
    qkv_w = gather(w_qkv.reshape(width, 3 * local).T)
    out_w = gather(w_out, qkv_w[2])
    up_w = gather(w_up, out_w[2])
    down_w = gather(w_down, up_w[2])
    bq = [b[:local] for b in biases]
    bv = [b[local : 2 * local] for b in biases]
    bu = [b[2 * local :] for b in biases]

    def pad(value):
        split = value.reshape(images, PATCHES, -1)
        return jnp.pad(split, ((0, 0), (0, PADDED - PATCHES), (0, 0))).reshape(images * PADDED, -1)

    def unpad(value):
        return value.reshape(images, PADDED, -1)[:, :PATCHES].reshape(rows, -1)

    classes = lax.dynamic_slice_in_dim(res_class, place * images, images)
    counts = jnp.where(classes == 0, PATCHES, PATCHES_LOW)
    key_valid = jnp.arange(PADDED)[None, :] < counts[:, None]
    row_valid = key_valid.reshape(-1).astype(F32)[:, None]

    inputs = pad(tokens).astype(F32)
    normed_a, factor_a = normalize(inputs)
    in_attn = (normed_a * gain_attn + shift_attn).astype(BF16)

    zero = jnp.zeros((group,), F32)
    saved = []
    branch = bias_out
    for g in range(2):
        pair = (2 * g, 2 * g + 1)
        w_pair = jnp.concatenate(
            [qkv_w[r][i * local : (i + 1) * local] for i in range(3) for r in pair], axis=0
        )
        out_pair = jnp.concatenate([out_w[r] for r in pair], axis=0)
        bias = jnp.concatenate([bq[pair[0]], bq[pair[1]], zero, bv[pair[0]], bv[pair[1]]])
        qkv = (dot(in_attn, w_pair, NT) + bias).astype(BF16)
        context, probs = attend(counts, qkv)
        branch = branch + dot(context, out_pair, NN)
        saved.append((w_pair, out_pair, qkv, context, probs))
    hidden = inputs + branch
    normed_m, factor_m = normalize(hidden)
    in_mlp = (normed_m * gain_mlp + shift_mlp).astype(BF16)
    acts = []
    slopes = []
    mlp = bias_down
    for r in range(4):
        pre = dot(in_mlp, up_w[r], NN) + bu[r]
        cdf = 0.5 * (1.0 + lax.erf(pre * (2.0 ** -0.5)))
        acts.append((pre * cdf).astype(BF16))
        slopes.append((cdf + pre * jnp.exp(-0.5 * pre * pre) * 0.3989422804014327).astype(BF16))
        mlp = mlp + dot(acts[r], down_w[r], NN)
    stream = (hidden + mlp) * row_valid
    block_out = unpad(stream.astype(BF16))

    def scatter(parts):
        near = parts[0] + swap(parts[1], "tensor", 1)
        far = parts[2] + swap(parts[3], "tensor", 1)
        return near + swap(far, "tensor", 2)

    dp_size = lax.axis_size("dp")
    dp_place = lax.axis_index("dp")
    bits = []
    while (1 << len(bits)) < dp_size:
        bits.append(len(bits))

    def high(bit):
        return (dp_place >> bit) % 2 == 1

    def halve(value, bit):
        rows_half = value.shape[0] // 2
        low_half, high_half = value[:rows_half], value[rows_half:]
        sent = jnp.where(high(bit), low_half, high_half)
        kept = jnp.where(high(bit), high_half, low_half)
        return kept + swap(sent, "dp", 1 << bit)

    def double(value, bit):
        other = swap(value, "dp", 1 << bit)
        return jnp.where(
            high(bit),
            jnp.concatenate([other, value], axis=0),
            jnp.concatenate([value, other], axis=0),
        )

    def finish(value, order):
        for bit in reversed(order):
            value = double(value, bit)
        return value

    y_first = bits
    z_first = bits[1:] + bits[:1]

    grad_stream = pad(cotangent).astype(F32) * row_valid
    grad_low = grad_stream.astype(BF16)
    grad_bias_down = jnp.sum(grad_stream, axis=0)
    d_down = [dot(acts[r], grad_low, TN).astype(BF16) for r in range(4)]
    grad_low = after(grad_low, *d_down)
    down_1 = swap(d_down[1], "tensor", 1)
    down_3 = swap(d_down[3], "tensor", 1)
    down = None
    d_bias_up, grads_pre = [], []
    grad_in_mlp = 0.0
    for r in range(4):
        if r == 2:
            grad_low = after(grad_low, down_1, down_3, grads_pre[1])
            down_far = swap(d_down[2] + down_3, "tensor", 2)
        grad_pre = dot(grad_low, down_w[r], NT) * slopes[r].astype(F32)
        d_bias_up.append(jnp.sum(grad_pre, axis=0))
        grads_pre.append(grad_pre.astype(BF16))
    d_up = [dot(in_mlp, grads_pre[r], TN).astype(BF16) for r in range(4)]
    in_order = after(grads_pre[0], *d_up)
    up_1 = swap(d_up[1], "tensor", 1)
    up_3 = swap(d_up[3], "tensor", 1)
    for r in range(4):
        grad_in_mlp = grad_in_mlp + dot(in_order if r == 0 else grads_pre[r], up_w[r], NT)

    grad_gain_mlp = jnp.sum(grad_in_mlp * normed_m, axis=0)
    grad_shift_mlp = jnp.sum(grad_in_mlp, axis=0)
    grad_hidden = grad_stream + norm_back(grad_in_mlp, gain_mlp, normed_m, factor_m)
    grad_bias_out = jnp.sum(grad_hidden, axis=0)
    grad_branch = after(grad_hidden.astype(BF16), up_1, up_3, down_far)
    up_far = swap(d_up[2] + up_3, "tensor", 2)
    down = halve(d_down[0] + down_1 + down_far, y_first[0])

    d_attn, d_bias_qv = [None] * 4, [None] * 4
    grad_in_attn = 0.0
    for g in (1, 0):
        w_pair, out_pair, qkv, context, probs = saved[g]
        if g == 0:
            grad_branch = after(grad_branch, down, far_attn)
            for bit in y_first[1:]:
                down = halve(down, bit)
        out_grad = dot(context, grad_branch, TN).astype(BF16)
        grad_context = dot(grad_branch, out_pair, NT).astype(BF16)
        low = attend_back(qkv, probs, grad_context)
        bias_sum = jnp.sum(low.astype(F32), axis=0).reshape(3, 2, local)
        qkv_grad = dot(low, in_attn, TN).astype(BF16)
        for k in range(2):
            r = 2 * g + k
            blocks = [qkv_grad[(2 * i + k) * local : (2 * i + k + 1) * local] for i in range(3)]
            d_attn[r] = jnp.concatenate(blocks + [out_grad[k * local : (k + 1) * local]], axis=0)
            d_bias_qv[r] = jnp.concatenate([bias_sum[0, k], bias_sum[2, k]])
        if g == 1:
            far_attn = d_attn[2] + swap(d_attn[3], "tensor", 1)
        grad_in_attn = grad_in_attn + dot(low, w_pair, NN)
    got_far = swap(far_attn, "tensor", 2)
    up = d_up[0] + up_1 + up_far
    up = halve(up, z_first[0])
    grad_in_attn, down, _ = lax.optimization_barrier((grad_in_attn, down, up))
    for bit in z_first[1:]:
        up = halve(up, bit)
    own_down = finish(down, y_first)
    own_up = finish(up, z_first)
    attn = d_attn[0] + swap(d_attn[1], "tensor", 1) + got_far
    half = attn.shape[0] // 2
    pieces = []
    for piece, order in ((attn[:half], y_first), (attn[half:], z_first)):
        for bit in order:
            piece = halve(piece, bit)
        pieces.append(finish(piece, order))
    own_attn = jnp.concatenate(pieces, axis=0).astype(F32)
    own_qkv = own_attn[: 3 * local].T.reshape(width, 3, local)
    own_out = own_attn[3 * local :]
    grad_gain_attn = jnp.sum(grad_in_attn * normed_a, axis=0)
    grad_shift_attn = jnp.sum(grad_in_attn, axis=0)
    grad_tokens = unpad(grad_hidden + norm_back(grad_in_attn, gain_attn, normed_a, factor_a))
    totals = jnp.stack(
        [
            jnp.sum(stream * stream),
            jnp.sum(branch * branch * row_valid),
            jnp.sum(mlp * mlp * row_valid),
            jnp.sum(row_valid),
        ]
    )
    shared = jnp.concatenate(
        [
            grad_gain_attn,
            grad_shift_attn,
            grad_bias_out,
            grad_gain_mlp,
            grad_shift_mlp,
            grad_bias_down,
            totals,
        ]
    )
    shared = shared + swap(shared, "tensor", 1)
    shared = shared + swap(shared, "tensor", 2)
    biases = scatter([jnp.concatenate([d_bias_qv[r], d_bias_up[r]]) for r in range(4)])
    small = jnp.concatenate([biases, shared])
    bit = 1
    while bit < lax.axis_size("dp"):
        small = small + swap(small, "dp", bit)
        bit *= 2
    wide = 2 * local + ff_local
    got = [small[wide + i * width : wide + (i + 1) * width] for i in range(6)]
    sums = small[wide + 6 * width :]
    rms = jnp.sqrt(sums[:3] / (sums[3] * width))
    return (
        block_out,
        grad_tokens,
        got[0],
        got[1],
        own_qkv,
        small[: 2 * local].reshape(2, local),
        own_out,
        got[2],
        got[3],
        got[4],
        own_up.astype(F32),
        small[2 * local : wide],
        own_down.astype(F32),
        got[5],
        rms,
    )


def solution(mesh):
    row = P(("dp", "tensor"), None)
    in_specs = (
        row, P("dp"), P(), P(), P(None, None, "tensor"), P(None, "tensor"), P("tensor", None),
        P(), P(), P(), P(None, "tensor"), P("tensor"), P("tensor", None), P(), row,
    )
    out_specs = (
        row, row, P(), P(), P(None, None, "tensor"), P(None, "tensor"), P("tensor", None),
        P(), P(), P(), P(None, "tensor"), P("tensor"), P("tensor", None), P(), P(),
    )
    return jax.shard_map(
        on_device, mesh=mesh, in_specs=in_specs, out_specs=out_specs, check_vma=False
    )
```

```python
import functools

import jax
import jax.numpy as jnp
from jax import lax
from jax.experimental import pallas as pl
from jax.experimental.pallas import tpu as pltpu
from jax.sharding import PartitionSpec as P


HEAD_DIM = 64
PATCHES = 196
PATCHES_LOW = 144
PADDED = 208
LANES = 128
EPS = 1e-06
F32 = jnp.float32
BF16 = jnp.bfloat16


def normalize(values):
    mean = jnp.mean(values, axis=-1, keepdims=True)
    centred = values - mean
    factor = lax.rsqrt(jnp.mean(centred * centred, axis=-1, keepdims=True) + EPS)
    return (centred * factor, factor)


def norm_back(grad_out, gain, normed, factor):
    scaled = grad_out * gain
    return factor * (
        scaled
        - jnp.mean(scaled, axis=-1, keepdims=True)
        - normed * jnp.mean(scaled * normed, axis=-1, keepdims=True)
    )


def dot(a, b, dims):
    return lax.dot_general(a, b, (dims, ((), ())), preferred_element_type=F32)


NN = ((1,), (0,))
NT = ((1,), (1,))
TN = ((0,), (0,))


def head_masks(factor):
    lane = lax.broadcasted_iota(jnp.int32, (1, LANES), 1)
    first = jnp.where(lane < HEAD_DIM, factor, 0.0)
    return first.astype(BF16), (factor - first).astype(BF16)


def attend_kernel(group, counts, qkv, context, probs):
    rows = qkv.shape[0]
    valid = counts[pl.program_id(0)]
    keep = lax.broadcasted_iota(jnp.int32, (rows, rows), 1) < valid
    ones = head_masks(1.0)
    scaled = head_masks(HEAD_DIM ** (-0.5))
    for j in range(group // LANES):
        at = j * LANES
        query = qkv[:, at : at + LANES]
        key = qkv[:, group + at : group + at + LANES]
        value = qkv[:, 2 * group + at : 2 * group + at + LANES]
        total = None
        for h in range(2):
            scores = dot(query * scaled[h], key, NT)
            scores = jnp.where(keep, scores, -1e30)
            top = jnp.max(scores, axis=-1, keepdims=True)
            raised = jnp.exp(scores - top)
            low = (raised * (1.0 / jnp.sum(raised, axis=-1, keepdims=True))).astype(BF16)
            probs[0, 2 * j + h] = low
            part = dot(low, value * ones[h], NN)
            total = part if total is None else total + part
        context[:, at : at + LANES] = total.astype(BF16)


def attend_back_kernel(group, qkv, probs, grad_context, grads):
    ones = head_masks(1.0)
    scaled = head_masks(HEAD_DIM ** (-0.5))
    for j in range(group // LANES):
        at = j * LANES
        query = qkv[:, at : at + LANES]
        key = qkv[:, group + at : group + at + LANES]
        value = qkv[:, 2 * group + at : 2 * group + at + LANES]
        grad = grad_context[:, at : at + LANES]
        sums = None
        for h in range(2):
            own = grad * ones[h]
            low = probs[0, 2 * j + h]
            wide = low.astype(F32)
            grad_probs = dot(own, value, NT)
            row_dot = jnp.sum(wide * grad_probs, axis=-1, keepdims=True)
            grad_scores = (wide * (grad_probs - row_dot)).astype(BF16)
            parts = (
                dot(grad_scores, key * scaled[h], NN),
                dot(grad_scores, query * scaled[h], TN),
                dot(low, own, TN),
            )
            sums = parts if sums is None else [a + b for a, b in zip(sums, parts)]
        for i in range(3):
            grads[:, i * group + at : i * group + at + LANES] = sums[i].astype(BF16)


def prepare_kernel(counts, tokens, cotangent, gain, shift, inputs, in_attn, grads):
    values = tokens[...].astype(F32)
    weights = cotangent[...].astype(F32)
    width = values.shape[1]
    fill = jnp.zeros((PADDED - PATCHES, width), F32)
    row = lax.broadcasted_iota(jnp.int32, (PADDED, 1), 0)
    for k in range(values.shape[0] // PATCHES):
        here = slice(k * PATCHES, (k + 1) * PATCHES)
        there = slice(k * PADDED, (k + 1) * PADDED)
        padded = jnp.concatenate([values[here], fill], axis=0)
        inputs[there] = padded
        in_attn[there] = (normalize(padded)[0] * gain[...] + shift[...]).astype(BF16)
        keep = row < counts[pl.program_id(0) * (values.shape[0] // PATCHES) + k]
        padded = jnp.concatenate([weights[here], fill], axis=0)
        grads[there] = jnp.where(keep, padded, 0.0).astype(BF16)


def prepare(counts, tokens, cotangent, gain, shift):
    rows, width = tokens.shape
    images = counts.shape[0]
    step = 2 if images % 2 == 0 else images
    source = pl.BlockSpec((step * PATCHES, width), lambda i, c: (i, 0))
    target = pl.BlockSpec((step * PADDED, width), lambda i, c: (i, 0))
    vector = pl.BlockSpec((1, width), lambda i, c: (0, 0))
    shape = (images * PADDED, width)
    return pl.pallas_call(
        prepare_kernel,
        grid_spec=pltpu.PrefetchScalarGridSpec(
            num_scalar_prefetch=1,
            grid=(images // step,),
            in_specs=[source, source, vector, vector],
            out_specs=[target, target, target],
        ),
        out_shape=[
            jax.ShapeDtypeStruct(shape, F32),
            jax.ShapeDtypeStruct(shape, BF16),
            jax.ShapeDtypeStruct(shape, BF16),
        ],
        cost_estimate=pl.CostEstimate(
            flops=rows * width * 20, bytes_accessed=rows * width * 12, transcendentals=0
        ),
        name="prepare",
    )(counts, tokens, cotangent, gain[None], shift[None])


def attend(counts, qkv):
    images = counts.shape[0]
    rows = qkv.shape[0] // images
    group = qkv.shape[1] // 3
    heads = group // HEAD_DIM
    return pl.pallas_call(
        functools.partial(attend_kernel, group),
        grid_spec=pltpu.PrefetchScalarGridSpec(
            num_scalar_prefetch=1,
            grid=(images,),
            in_specs=[pl.BlockSpec((rows, 3 * group), lambda i, c: (i, 0))],
            out_specs=[
                pl.BlockSpec((rows, group), lambda i, c: (i, 0)),
                pl.BlockSpec((1, heads, rows, rows), lambda i, c: (i, 0, 0, 0)),
            ],
        ),
        out_shape=[
            jax.ShapeDtypeStruct((images * rows, group), BF16),
            jax.ShapeDtypeStruct((images, heads, rows, rows), BF16),
        ],
        cost_estimate=pl.CostEstimate(
            flops=images * heads * rows * rows * HEAD_DIM * 16,
            bytes_accessed=images * rows * group * 8,
            transcendentals=images * heads * rows * rows,
        ),
        name="attend",
    )(counts, qkv)


def attend_back(qkv, probs, grad_context):
    images, heads, rows, _ = probs.shape
    group = qkv.shape[1] // 3
    wide = pl.BlockSpec((rows, 3 * group), lambda i: (i, 0))
    return pl.pallas_call(
        functools.partial(attend_back_kernel, group),
        grid=(images,),
        in_specs=[
            wide,
            pl.BlockSpec((1, heads, rows, rows), lambda i: (i, 0, 0, 0)),
            pl.BlockSpec((rows, group), lambda i: (i, 0)),
        ],
        out_specs=wide,
        out_shape=jax.ShapeDtypeStruct(qkv.shape, BF16),
        cost_estimate=pl.CostEstimate(
            flops=images * heads * rows * rows * HEAD_DIM * 40,
            bytes_accessed=images * rows * group * 16,
            transcendentals=0,
        ),
        name="attend_back",
    )(qkv, probs, grad_context)


def swap(value, axis, bit):
    size = lax.axis_size(axis)
    return lax.ppermute(value, axis, [(i, i ^ bit) for i in range(size)])


def after(value, *earlier):
    return lax.optimization_barrier((value, *earlier))[0]


def on_device(
    tokens,
    res_class,
    gain_attn,
    shift_attn,
    w_qkv,
    bias_qv,
    w_out,
    bias_out,
    gain_mlp,
    shift_mlp,
    w_up,
    bias_up,
    w_down,
    bias_down,
    cotangent,
):
    rows, width = tokens.shape
    local = w_qkv.shape[2]
    images = rows // PATCHES
    place = lax.axis_index("tensor")
    ff_local = w_up.shape[1]
    group = 2 * local

    def gather(value):
        far = swap(value, "tensor", 2)
        return [value, swap(value, "tensor", 1), far, swap(far, "tensor", 1)]

    biases = gather(jnp.concatenate([bias_qv.reshape(-1), bias_up]))
    qkv_w = gather(w_qkv.reshape(width, 3 * local).T)
    out_w = gather(w_out)
    up_w = gather(w_up)
    down_w = gather(w_down)
    bq = [b[:local] for b in biases]
    bv = [b[local : 2 * local] for b in biases]
    bu = [b[2 * local :] for b in biases]

    def unpad(value):
        return value.reshape(images, PADDED, -1)[:, :PATCHES].reshape(rows, -1)

    classes = lax.dynamic_slice_in_dim(res_class, place * images, images)
    counts = jnp.where(classes == 0, PATCHES, PATCHES_LOW)
    key_valid = jnp.arange(PADDED)[None, :] < counts[:, None]
    row_valid = key_valid.reshape(-1).astype(F32)[:, None]

    inputs, in_attn, grad_low = prepare(counts, tokens, cotangent, gain_attn, shift_attn)

    zero = jnp.zeros((group,), F32)
    saved = []
    branch = bias_out
    for g in range(2):
        pair = (2 * g, 2 * g + 1)
        w_pair = jnp.concatenate([qkv_w[r].reshape(3, local, width) for r in pair], axis=1)
        w_pair = w_pair.reshape(3 * group, width)
        out_pair = jnp.concatenate([out_w[r] for r in pair], axis=0)
        bias = jnp.concatenate([bq[pair[0]], bq[pair[1]], zero, bv[pair[0]], bv[pair[1]]])
        qkv = (dot(in_attn, w_pair, NT) + bias).astype(BF16)
        context, probs = attend(counts, qkv)
        branch = branch + dot(context, out_pair, NN)
        saved.append((w_pair, out_pair, qkv, context, probs))
    hidden = inputs + branch
    normed_m, factor_m = normalize(hidden)
    in_mlp = lax.optimization_barrier((normed_m * gain_mlp + shift_mlp).astype(BF16))
    acts = []
    slopes = []
    mlp = bias_down
    for r in range(4):
        up_in = in_mlp if r == 0 else after(in_mlp, acts[r - 1])
        pre = dot(up_in, up_w[r], NN) + bu[r]
        cdf = 0.5 * (1.0 + lax.erf(pre * (2.0 ** -0.5)))
        acts.append((pre * cdf).astype(BF16))
        slopes.append((cdf + pre * jnp.exp(-0.5 * pre * pre) * 0.3989422804014327).astype(BF16))
        mlp = mlp + dot(acts[r], down_w[r], NN)
    stream = (hidden + mlp) * row_valid
    block_out = unpad(stream.astype(BF16))

    def scatter(parts):
        near = parts[0] + swap(parts[1], "tensor", 1)
        far = parts[2] + swap(parts[3], "tensor", 1)
        return near + swap(far, "tensor", 2)

    dp_size = lax.axis_size("dp")
    dp_place = lax.axis_index("dp")
    bits = []
    while (1 << len(bits)) < dp_size:
        bits.append(len(bits))

    def high(bit):
        return (dp_place >> bit) % 2 == 1

    def halve(value, bit):
        rows_half = value.shape[0] // 2
        low_half, high_half = value[:rows_half], value[rows_half:]
        sent = jnp.where(high(bit), low_half, high_half)
        kept = jnp.where(high(bit), high_half, low_half)
        return kept + swap(sent, "dp", 1 << bit)

    def double(value, bit):
        other = swap(value, "dp", 1 << bit)
        return jnp.where(
            high(bit),
            jnp.concatenate([other, value], axis=0),
            jnp.concatenate([value, other], axis=0),
        )

    def finish(value, order):
        for bit in reversed(order):
            value = double(value, bit)
        return value

    y_first = bits
    z_first = bits[1:] + bits[:1]

    grad_stream = grad_low.astype(F32)
    grad_bias_down = jnp.sum(grad_stream, axis=0)
    d_down = [dot(acts[r], grad_low, TN).astype(BF16) for r in range(4)]
    grad_low = after(grad_low, *d_down)
    down_1 = swap(d_down[1], "tensor", 1)
    down_3 = swap(d_down[3], "tensor", 1)
    down_far = swap(d_down[2] + down_3, "tensor", 2)
    d_bias_up, grads_pre, d_up = [], [], []
    grad_in_mlp = 0.0
    for r in range(4):
        back_in = grad_low if r == 0 else after(grad_low, grads_pre[r - 1])
        grad_pre = dot(back_in, down_w[r], NT) * slopes[r].astype(F32)
        d_bias_up.append(jnp.sum(grad_pre, axis=0))
        grads_pre.append(grad_pre.astype(BF16))
    up_in = after(in_mlp, grads_pre[3])
    for r in (3, 2, 1, 0):
        d_up.append(dot(up_in, grads_pre[r], TN).astype(BF16))
    d_up = d_up[::-1]
    up_1 = swap(d_up[1], "tensor", 1)
    up_3 = swap(d_up[3], "tensor", 1)
    grads_pre[0] = after(grads_pre[0], *d_up)
    for r in range(4):
        grad_in_mlp = grad_in_mlp + dot(grads_pre[r], up_w[r], NT)
    up_far = swap(d_up[2] + up_3, "tensor", 2)

    grad_gain_mlp = jnp.sum(grad_in_mlp * normed_m, axis=0)
    grad_shift_mlp = jnp.sum(grad_in_mlp, axis=0)
    grad_hidden = grad_stream + norm_back(grad_in_mlp, gain_mlp, normed_m, factor_m)
    grad_bias_out = jnp.sum(grad_hidden, axis=0)
    grad_branch = grad_hidden.astype(BF16)
    down = d_down[0] + down_1 + down_far
    for bit in y_first:
        down = halve(down, bit)
    up = d_up[0] + up_1 + up_far
    for bit in z_first:
        up = halve(up, bit)

    d_attn, d_bias_qv, lows = [None] * 4, [None] * 4, [None] * 2
    for g in (1, 0):
        w_pair, out_pair, qkv, context, probs = saved[g]
        out_grad = dot(context, grad_branch, TN).astype(BF16)
        grad_context = dot(grad_branch, out_pair, NT).astype(BF16)
        low = attend_back(qkv, probs, grad_context)
        lows[g] = low
        qkv_grad = dot(low, in_attn, TN).astype(BF16)
        grad_branch = after(grad_branch, qkv_grad)
        bias_sum = jnp.sum(low.astype(F32), axis=0).reshape(3, 2, local)
        for k in range(2):
            r = 2 * g + k
            blocks = [qkv_grad[(2 * i + k) * local : (2 * i + k + 1) * local] for i in range(3)]
            d_attn[r] = jnp.concatenate(blocks + [out_grad[k * local : (k + 1) * local]], axis=0)
            d_bias_qv[r] = jnp.concatenate([bias_sum[0, k], bias_sum[2, k]])
    far_attn = d_attn[2] + swap(d_attn[3], "tensor", 1)
    got_far = swap(far_attn, "tensor", 2)
    lows = lax.optimization_barrier((lows[0], lows[1], qkv_grad))[:2]
    grad_in_attn = dot(lows[0], saved[0][0], NN)
    grad_in_attn = grad_in_attn + dot(lows[1], saved[1][0], NN)
    own_down = finish(down, y_first)
    own_up = finish(up, z_first)
    attn = d_attn[0] + swap(d_attn[1], "tensor", 1) + got_far
    half = attn.shape[0] // 2
    pieces = []
    for piece, order in ((attn[:half], y_first), (attn[half:], z_first)):
        for bit in order:
            piece = halve(piece, bit)
        pieces.append(finish(piece, order))
    own_attn = jnp.concatenate(pieces, axis=0).astype(F32)
    own_qkv = own_attn[: 3 * local].T.reshape(width, 3, local)
    own_out = own_attn[3 * local :]
    normed_a, factor_a = normalize(after(inputs, qkv_grad))
    grad_gain_attn = jnp.sum(grad_in_attn * normed_a, axis=0)
    grad_shift_attn = jnp.sum(grad_in_attn, axis=0)
    grad_tokens = grad_hidden + norm_back(grad_in_attn, gain_attn, normed_a, factor_a)
    grad_tokens = unpad(grad_tokens)
    totals = jnp.stack(
        [
            jnp.sum(stream * stream),
            jnp.sum(branch * branch * row_valid),
            jnp.sum(mlp * mlp * row_valid),
            jnp.sum(row_valid),
        ]
    )
    shared = jnp.concatenate(
        [
            grad_gain_attn,
            grad_shift_attn,
            grad_bias_out,
            grad_gain_mlp,
            grad_shift_mlp,
            grad_bias_down,
            totals,
        ]
    )
    shared = after(shared, attn)
    shared = shared + swap(shared, "tensor", 1)
    shared = shared + swap(shared, "tensor", 2)
    biases = scatter([jnp.concatenate([d_bias_qv[r], d_bias_up[r]]) for r in range(4)])
    small = jnp.concatenate([biases, shared])
    bit = 1
    while bit < lax.axis_size("dp"):
        small = small + swap(small, "dp", bit)
        bit *= 2
    wide = 2 * local + ff_local
    got = [small[wide + i * width : wide + (i + 1) * width] for i in range(6)]
    sums = small[wide + 6 * width :]
    rms = jnp.sqrt(sums[:3] / (sums[3] * width))
    return (
        block_out,
        grad_tokens,
        got[0],
        got[1],
        own_qkv,
        small[: 2 * local].reshape(2, local),
        own_out,
        got[2],
        got[3],
        got[4],
        own_up.astype(F32),
        small[2 * local : wide],
        own_down.astype(F32),
        got[5],
        rms,
    )


def solution(mesh):
    row = P(("dp", "tensor"), None)
    in_specs = (
        row, P("dp"), P(), P(), P(None, None, "tensor"), P(None, "tensor"), P("tensor", None),
        P(), P(), P(), P(None, "tensor"), P("tensor"), P("tensor", None), P(), row,
    )
    out_specs = (
        row, row, P(), P(), P(None, None, "tensor"), P(None, "tensor"), P("tensor", None),
        P(), P(), P(), P(None, "tensor"), P("tensor"), P("tensor", None), P(), P(),
    )
    return jax.shard_map(
        on_device, mesh=mesh, in_specs=in_specs, out_specs=out_specs, check_vma=False
    )
```

```python
import functools

import jax
import jax.numpy as jnp
from jax import lax
from jax.experimental import pallas as pl
from jax.experimental.pallas import tpu as pltpu
from jax.sharding import PartitionSpec as P


HEAD_DIM = 64
PATCHES = 196
PATCHES_LOW = 144
PADDED = 208
LANES = 128
EPS = 1e-06
F32 = jnp.float32
BF16 = jnp.bfloat16


def normalize(values):
    mean = jnp.mean(values, axis=-1, keepdims=True)
    centred = values - mean
    factor = lax.rsqrt(jnp.mean(centred * centred, axis=-1, keepdims=True) + EPS)
    return (centred * factor, factor)


def norm_back(grad_out, gain, normed, factor):
    scaled = grad_out * gain
    return factor * (
        scaled
        - jnp.mean(scaled, axis=-1, keepdims=True)
        - normed * jnp.mean(scaled * normed, axis=-1, keepdims=True)
    )


def dot(a, b, dims):
    return lax.dot_general(a, b, (dims, ((), ())), preferred_element_type=F32)


NN = ((1,), (0,))
NT = ((1,), (1,))
TN = ((0,), (0,))


def head_masks(factor):
    lane = lax.broadcasted_iota(jnp.int32, (1, LANES), 1)
    first = jnp.where(lane < HEAD_DIM, factor, 0.0)
    return first.astype(BF16), (factor - first).astype(BF16)


def attend_kernel(group, counts, qkv, context, probs):
    rows = qkv.shape[0]
    valid = counts[pl.program_id(0)]
    keep = lax.broadcasted_iota(jnp.int32, (rows, rows), 1) < valid
    ones = head_masks(1.0)
    scaled = head_masks(HEAD_DIM ** (-0.5))
    for j in range(group // LANES):
        at = j * LANES
        query = qkv[:, at : at + LANES]
        key = qkv[:, group + at : group + at + LANES]
        value = qkv[:, 2 * group + at : 2 * group + at + LANES]
        total = None
        for h in range(2):
            scores = dot(query * scaled[h], key, NT)
            scores = jnp.where(keep, scores, -1e30)
            top = jnp.max(scores, axis=-1, keepdims=True)
            raised = jnp.exp(scores - top)
            low = (raised * (1.0 / jnp.sum(raised, axis=-1, keepdims=True))).astype(BF16)
            probs[0, 2 * j + h] = low
            part = dot(low, value * ones[h], NN)
            total = part if total is None else total + part
        context[:, at : at + LANES] = total.astype(BF16)


def attend_back_kernel(group, qkv, probs, grad_context, grads):
    ones = head_masks(1.0)
    scaled = head_masks(HEAD_DIM ** (-0.5))
    for j in range(group // LANES):
        at = j * LANES
        query = qkv[:, at : at + LANES]
        key = qkv[:, group + at : group + at + LANES]
        value = qkv[:, 2 * group + at : 2 * group + at + LANES]
        grad = grad_context[:, at : at + LANES]
        sums = None
        for h in range(2):
            own = grad * ones[h]
            low = probs[0, 2 * j + h]
            wide = low.astype(F32)
            grad_probs = dot(own, value, NT)
            row_dot = jnp.sum(wide * grad_probs, axis=-1, keepdims=True)
            grad_scores = (wide * (grad_probs - row_dot)).astype(BF16)
            parts = (
                dot(grad_scores, key * scaled[h], NN),
                dot(grad_scores, query * scaled[h], TN),
                dot(low, own, TN),
            )
            sums = parts if sums is None else [a + b for a, b in zip(sums, parts)]
        for i in range(3):
            grads[:, i * group + at : i * group + at + LANES] = sums[i].astype(BF16)


def prepare_kernel(counts, tokens, cotangent, gain, shift, inputs, in_attn, grads):
    values = tokens[...].astype(F32)
    weights = cotangent[...].astype(F32)
    width = values.shape[1]
    fill = jnp.zeros((PADDED - PATCHES, width), F32)
    row = lax.broadcasted_iota(jnp.int32, (PADDED, 1), 0)
    for k in range(values.shape[0] // PATCHES):
        here = slice(k * PATCHES, (k + 1) * PATCHES)
        there = slice(k * PADDED, (k + 1) * PADDED)
        padded = jnp.concatenate([values[here], fill], axis=0)
        inputs[there] = padded
        in_attn[there] = (normalize(padded)[0] * gain[...] + shift[...]).astype(BF16)
        keep = row < counts[pl.program_id(0) * (values.shape[0] // PATCHES) + k]
        padded = jnp.concatenate([weights[here], fill], axis=0)
        grads[there] = jnp.where(keep, padded, 0.0).astype(BF16)


def prepare(counts, tokens, cotangent, gain, shift):
    rows, width = tokens.shape
    images = counts.shape[0]
    step = 2 if images % 2 == 0 else images
    source = pl.BlockSpec((step * PATCHES, width), lambda i, c: (i, 0))
    target = pl.BlockSpec((step * PADDED, width), lambda i, c: (i, 0))
    vector = pl.BlockSpec((1, width), lambda i, c: (0, 0))
    shape = (images * PADDED, width)
    return pl.pallas_call(
        prepare_kernel,
        grid_spec=pltpu.PrefetchScalarGridSpec(
            num_scalar_prefetch=1,
            grid=(images // step,),
            in_specs=[source, source, vector, vector],
            out_specs=[target, target, target],
        ),
        out_shape=[
            jax.ShapeDtypeStruct(shape, F32),
            jax.ShapeDtypeStruct(shape, BF16),
            jax.ShapeDtypeStruct(shape, BF16),
        ],
        cost_estimate=pl.CostEstimate(
            flops=rows * width * 20, bytes_accessed=rows * width * 12, transcendentals=0
        ),
        name="prepare",
    )(counts, tokens, cotangent, gain[None], shift[None])


def attend(counts, qkv):
    images = counts.shape[0]
    rows = qkv.shape[0] // images
    group = qkv.shape[1] // 3
    heads = group // HEAD_DIM
    return pl.pallas_call(
        functools.partial(attend_kernel, group),
        grid_spec=pltpu.PrefetchScalarGridSpec(
            num_scalar_prefetch=1,
            grid=(images,),
            in_specs=[pl.BlockSpec((rows, 3 * group), lambda i, c: (i, 0))],
            out_specs=[
                pl.BlockSpec((rows, group), lambda i, c: (i, 0)),
                pl.BlockSpec((1, heads, rows, rows), lambda i, c: (i, 0, 0, 0)),
            ],
        ),
        out_shape=[
            jax.ShapeDtypeStruct((images * rows, group), BF16),
            jax.ShapeDtypeStruct((images, heads, rows, rows), BF16),
        ],
        cost_estimate=pl.CostEstimate(
            flops=images * heads * rows * rows * HEAD_DIM * 16,
            bytes_accessed=images * rows * group * 8,
            transcendentals=images * heads * rows * rows,
        ),
        name="attend",
    )(counts, qkv)


def attend_back(qkv, probs, grad_context):
    images, heads, rows, _ = probs.shape
    group = qkv.shape[1] // 3
    wide = pl.BlockSpec((rows, 3 * group), lambda i: (i, 0))
    return pl.pallas_call(
        functools.partial(attend_back_kernel, group),
        grid=(images,),
        in_specs=[
            wide,
            pl.BlockSpec((1, heads, rows, rows), lambda i: (i, 0, 0, 0)),
            pl.BlockSpec((rows, group), lambda i: (i, 0)),
        ],
        out_specs=wide,
        out_shape=jax.ShapeDtypeStruct(qkv.shape, BF16),
        cost_estimate=pl.CostEstimate(
            flops=images * heads * rows * rows * HEAD_DIM * 40,
            bytes_accessed=images * rows * group * 16,
            transcendentals=0,
        ),
        name="attend_back",
    )(qkv, probs, grad_context)


def swap(value, axis, bit):
    size = lax.axis_size(axis)
    return lax.ppermute(value, axis, [(i, i ^ bit) for i in range(size)])


def after(value, *earlier):
    return lax.optimization_barrier((value, *earlier))[0]


def on_device(
    tokens,
    res_class,
    gain_attn,
    shift_attn,
    w_qkv,
    bias_qv,
    w_out,
    bias_out,
    gain_mlp,
    shift_mlp,
    w_up,
    bias_up,
    w_down,
    bias_down,
    cotangent,
):
    rows, width = tokens.shape
    local = w_qkv.shape[2]
    images = rows // PATCHES
    place = lax.axis_index("tensor")
    ff_local = w_up.shape[1]
    group = 2 * local

    def gather(value):
        far = swap(value, "tensor", 2)
        return [value, swap(value, "tensor", 1), far, swap(far, "tensor", 1)]

    biases = gather(jnp.concatenate([bias_qv.reshape(-1), bias_up]))
    qkv_w = gather(w_qkv.reshape(width, 3 * local).T)
    out_w = gather(w_out)
    up_w = gather(w_up)
    down_w = gather(w_down)
    bq = [b[:local] for b in biases]
    bv = [b[local : 2 * local] for b in biases]
    bu = [b[2 * local :] for b in biases]

    def unpad(value):
        return value.reshape(images, PADDED, -1)[:, :PATCHES].reshape(rows, -1)

    classes = lax.dynamic_slice_in_dim(res_class, place * images, images)
    counts = jnp.where(classes == 0, PATCHES, PATCHES_LOW)
    key_valid = jnp.arange(PADDED)[None, :] < counts[:, None]
    row_valid = key_valid.reshape(-1).astype(F32)[:, None]

    inputs, in_attn, grad_low = prepare(counts, tokens, cotangent, gain_attn, shift_attn)

    zero = jnp.zeros((group,), F32)
    saved = []
    branch = bias_out
    for g in range(2):
        pair = (2 * g, 2 * g + 1)
        w_pair = jnp.concatenate([qkv_w[r].reshape(3, local, width) for r in pair], axis=1)
        w_pair = w_pair.reshape(3 * group, width)
        out_pair = jnp.concatenate([out_w[r] for r in pair], axis=0)
        bias = jnp.concatenate([bq[pair[0]], bq[pair[1]], zero, bv[pair[0]], bv[pair[1]]])
        qkv = (dot(in_attn, w_pair, NT) + bias).astype(BF16)
        context, probs = attend(counts, qkv)
        branch = branch + dot(context, out_pair, NN)
        saved.append((w_pair, out_pair, qkv, context, probs))
    hidden = inputs + branch
    normed_m, factor_m = normalize(hidden)
    in_mlp = lax.optimization_barrier((normed_m * gain_mlp + shift_mlp).astype(BF16))
    acts = []
    slopes = []
    mlp = bias_down
    for r in range(4):
        up_in = in_mlp if r == 0 else after(in_mlp, acts[r - 1])
        pre = dot(up_in, up_w[r], NN) + bu[r]
        cdf = 0.5 * (1.0 + lax.erf(pre * (2.0 ** -0.5)))
        acts.append((pre * cdf).astype(BF16))
        slopes.append((cdf + pre * jnp.exp(-0.5 * pre * pre) * 0.3989422804014327).astype(BF16))
        mlp = mlp + dot(acts[r], down_w[r], NN)
    stream = (hidden + mlp) * row_valid
    block_out = unpad(stream.astype(BF16))

    def scatter(parts):
        near = parts[0] + swap(parts[1], "tensor", 1)
        far = parts[2] + swap(parts[3], "tensor", 1)
        return near + swap(far, "tensor", 2)

    dp_size = lax.axis_size("dp")
    dp_place = lax.axis_index("dp")
    bits = []
    while (1 << len(bits)) < dp_size:
        bits.append(len(bits))

    def high(bit):
        return (dp_place >> bit) % 2 == 1

    def halve(value, bit):
        rows_half = value.shape[0] // 2
        low_half, high_half = value[:rows_half], value[rows_half:]
        sent = jnp.where(high(bit), low_half, high_half)
        kept = jnp.where(high(bit), high_half, low_half)
        return kept + swap(sent, "dp", 1 << bit)

    def double(value, bit):
        other = swap(value, "dp", 1 << bit)
        return jnp.where(
            high(bit),
            jnp.concatenate([other, value], axis=0),
            jnp.concatenate([value, other], axis=0),
        )

    def finish(value, order):
        for bit in reversed(order):
            value = double(value, bit)
        return value

    y_first = bits

    grad_stream = grad_low.astype(F32)
    grad_bias_down = jnp.sum(grad_stream, axis=0)
    d_down = [dot(acts[r], grad_low, TN).astype(BF16) for r in range(4)]
    grad_low = after(grad_low, *d_down)
    down_1 = swap(d_down[1], "tensor", 1)
    down_3 = swap(d_down[3], "tensor", 1)
    down_far = swap(d_down[2] + down_3, "tensor", 2)
    d_bias_up, grads_pre, d_up = [], [], []
    grad_in_mlp = 0.0
    for r in range(4):
        back_in = grad_low if r == 0 else after(grad_low, grads_pre[r - 1])
        grad_pre = dot(back_in, down_w[r], NT) * slopes[r].astype(F32)
        d_bias_up.append(jnp.sum(grad_pre, axis=0))
        grads_pre.append(grad_pre.astype(BF16))
    up_in = after(in_mlp, grads_pre[3])
    for r in (3, 2, 1, 0):
        d_up.append(dot(up_in, grads_pre[r], TN).astype(BF16))
    d_up = d_up[::-1]
    up_1 = swap(d_up[1], "tensor", 1)
    up_3 = swap(d_up[3], "tensor", 1)
    grads_pre[0] = after(grads_pre[0], *d_up)
    for r in range(4):
        grad_in_mlp = grad_in_mlp + dot(grads_pre[r], up_w[r], NT)
    up_far = swap(d_up[2] + up_3, "tensor", 2)

    grad_gain_mlp = jnp.sum(grad_in_mlp * normed_m, axis=0)
    grad_shift_mlp = jnp.sum(grad_in_mlp, axis=0)
    grad_hidden = grad_stream + norm_back(grad_in_mlp, gain_mlp, normed_m, factor_m)
    grad_bias_out = jnp.sum(grad_hidden, axis=0)
    grad_branch = grad_hidden.astype(BF16)
    down = d_down[0] + down_1 + down_far
    for bit in y_first:
        down = halve(down, bit)
    up = d_up[0] + up_1 + up_far
    for bit in y_first:
        up = halve(up, bit)

    d_attn, d_bias_qv, lows = [None] * 4, [None] * 4, [None] * 2
    for g in (1, 0):
        w_pair, out_pair, qkv, context, probs = saved[g]
        out_grad = dot(context, grad_branch, TN).astype(BF16)
        grad_context = dot(grad_branch, out_pair, NT).astype(BF16)
        low = attend_back(qkv, probs, grad_context)
        lows[g] = low
        qkv_grad = dot(low, in_attn, TN).astype(BF16)
        grad_branch = after(grad_branch, qkv_grad)
        for k in range(2):
            r = 2 * g + k
            blocks = [qkv_grad[(2 * i + k) * local : (2 * i + k + 1) * local] for i in range(3)]
            d_attn[r] = jnp.concatenate(blocks + [out_grad[k * local : (k + 1) * local]], axis=0)
    far_attn = d_attn[2] + swap(d_attn[3], "tensor", 1)
    got_far = swap(far_attn, "tensor", 2)
    lows = lax.optimization_barrier((lows[0], lows[1], qkv_grad))[:2]
    grad_in_attn = dot(lows[0], saved[0][0], NN)
    grad_in_attn = grad_in_attn + dot(lows[1], saved[1][0], NN)
    own_down = finish(down, y_first)
    own_up = finish(up, y_first)
    attn = d_attn[0] + swap(d_attn[1], "tensor", 1) + got_far
    half = attn.shape[0] // 2
    pieces = []
    for piece, order in ((attn[:half], y_first), (attn[half:], y_first)):
        for bit in order:
            piece = halve(piece, bit)
        pieces.append(finish(piece, order))
    own_attn = jnp.concatenate(pieces, axis=0).astype(F32)
    own_qkv = own_attn[: 3 * local].T.reshape(width, 3, local)
    own_out = own_attn[3 * local :]
    late = lax.optimization_barrier((inputs, grad_in_attn, lows[0], lows[1], attn))
    inputs, grad_in_attn = late[:2]
    for g in range(2):
        bias_sum = jnp.sum(late[2 + g].astype(F32), axis=0).reshape(3, 2, local)
        for k in range(2):
            d_bias_qv[2 * g + k] = jnp.concatenate([bias_sum[0, k], bias_sum[2, k]])
    normed_a, factor_a = normalize(inputs)
    grad_gain_attn = jnp.sum(grad_in_attn * normed_a, axis=0)
    grad_shift_attn = jnp.sum(grad_in_attn, axis=0)
    grad_tokens = grad_hidden + norm_back(grad_in_attn, gain_attn, normed_a, factor_a)
    grad_tokens = unpad(grad_tokens)
    totals = jnp.stack(
        [
            jnp.sum(stream * stream),
            jnp.sum(branch * branch * row_valid),
            jnp.sum(mlp * mlp * row_valid),
            jnp.sum(row_valid),
        ]
    )
    shared = jnp.concatenate(
        [
            grad_gain_attn,
            grad_shift_attn,
            grad_bias_out,
            grad_gain_mlp,
            grad_shift_mlp,
            grad_bias_down,
            totals,
        ]
    )
    shared = after(shared, attn)
    shared = shared + swap(shared, "tensor", 1)
    shared = shared + swap(shared, "tensor", 2)
    biases = scatter([jnp.concatenate([d_bias_qv[r], d_bias_up[r]]) for r in range(4)])
    small = jnp.concatenate([biases, shared])
    for bit in bits:
        small = small + swap(small, "dp", 1 << bit)
    wide = 2 * local + ff_local
    got = [small[wide + i * width : wide + (i + 1) * width] for i in range(6)]
    sums = small[wide + 6 * width :]
    rms = jnp.sqrt(sums[:3] / (sums[3] * width))
    return (
        block_out,
        grad_tokens,
        got[0],
        got[1],
        own_qkv,
        small[: 2 * local].reshape(2, local),
        own_out,
        got[2],
        got[3],
        got[4],
        own_up.astype(F32),
        small[2 * local : wide],
        own_down.astype(F32),
        got[5],
        rms,
    )


def solution(mesh):
    row = P(("dp", "tensor"), None)
    in_specs = (
        row, P("dp"), P(), P(), P(None, None, "tensor"), P(None, "tensor"), P("tensor", None),
        P(), P(), P(), P(None, "tensor"), P("tensor"), P("tensor", None), P(), row,
    )
    out_specs = (
        row, row, P(), P(), P(None, None, "tensor"), P(None, "tensor"), P("tensor", None),
        P(), P(), P(), P(None, "tensor"), P("tensor"), P("tensor", None), P(), P(),
    )
    return jax.shard_map(
        on_device, mesh=mesh, in_specs=in_specs, out_specs=out_specs, check_vma=False
    )
```

```python
import functools

import jax
import jax.numpy as jnp
from jax import lax
from jax.experimental import pallas as pl
from jax.experimental.pallas import tpu as pltpu
from jax.sharding import PartitionSpec as P


HEAD_DIM = 64
PATCHES = 196
PATCHES_LOW = 144
PADDED = 208
LANES = 128
EPS = 1e-06
F32 = jnp.float32
BF16 = jnp.bfloat16


def normalize(values):
    mean = jnp.mean(values, axis=-1, keepdims=True)
    centred = values - mean
    factor = lax.rsqrt(jnp.mean(centred * centred, axis=-1, keepdims=True) + EPS)
    return (centred * factor, factor)


def norm_back(grad_out, gain, normed, factor):
    scaled = grad_out * gain
    return factor * (
        scaled
        - jnp.mean(scaled, axis=-1, keepdims=True)
        - normed * jnp.mean(scaled * normed, axis=-1, keepdims=True)
    )


def dot(a, b, dims):
    return lax.dot_general(a, b, (dims, ((), ())), preferred_element_type=F32)


NN = ((1,), (0,))
NT = ((1,), (1,))
TN = ((0,), (0,))


def head_masks(factor):
    lane = lax.broadcasted_iota(jnp.int32, (1, LANES), 1)
    first = jnp.where(lane < HEAD_DIM, factor, 0.0)
    return first.astype(BF16), (factor - first).astype(BF16)


def attend_kernel(group, counts, qkv, context, probs):
    rows = qkv.shape[0]
    valid = counts[pl.program_id(0)]
    keep = lax.broadcasted_iota(jnp.int32, (rows, rows), 1) < valid
    ones = head_masks(1.0)
    scaled = head_masks(HEAD_DIM ** (-0.5))
    for j in range(group // LANES):
        at = j * LANES
        query = qkv[:, at : at + LANES]
        key = qkv[:, group + at : group + at + LANES]
        value = qkv[:, 2 * group + at : 2 * group + at + LANES]
        total = None
        for h in range(2):
            scores = dot(query * scaled[h], key, NT)
            scores = jnp.where(keep, scores, -1e30)
            top = jnp.max(scores, axis=-1, keepdims=True)
            raised = jnp.exp(scores - top)
            low = (raised * (1.0 / jnp.sum(raised, axis=-1, keepdims=True))).astype(BF16)
            probs[0, 2 * j + h] = low
            part = dot(low, value * ones[h], NN)
            total = part if total is None else total + part
        context[:, at : at + LANES] = total.astype(BF16)


def attend_back_kernel(group, qkv, probs, grad_context, grads):
    ones = head_masks(1.0)
    scaled = head_masks(HEAD_DIM ** (-0.5))
    for j in range(group // LANES):
        at = j * LANES
        query = qkv[:, at : at + LANES]
        key = qkv[:, group + at : group + at + LANES]
        value = qkv[:, 2 * group + at : 2 * group + at + LANES]
        grad = grad_context[:, at : at + LANES]
        sums = None
        for h in range(2):
            own = grad * ones[h]
            low = probs[0, 2 * j + h]
            wide = low.astype(F32)
            grad_probs = dot(own, value, NT)
            row_dot = jnp.sum(wide * grad_probs, axis=-1, keepdims=True)
            grad_scores = (wide * (grad_probs - row_dot)).astype(BF16)
            parts = (
                dot(grad_scores, key * scaled[h], NN),
                dot(grad_scores, query * scaled[h], TN),
                dot(low, own, TN),
            )
            sums = parts if sums is None else [a + b for a, b in zip(sums, parts)]
        for i in range(3):
            grads[:, i * group + at : i * group + at + LANES] = sums[i].astype(BF16)


def prepare_kernel(counts, tokens, cotangent, affine, inputs, in_attn, grads):
    values = tokens[...].astype(F32)
    weights = cotangent[...].astype(F32)
    width = values.shape[1]
    fill = jnp.zeros((PADDED - PATCHES, width), F32)
    row = lax.broadcasted_iota(jnp.int32, (PADDED, 1), 0)
    for k in range(values.shape[0] // PATCHES):
        here = slice(k * PATCHES, (k + 1) * PATCHES)
        there = slice(k * PADDED, (k + 1) * PADDED)
        padded = jnp.concatenate([values[here], fill], axis=0)
        inputs[there] = padded
        in_attn[there] = (normalize(padded)[0] * affine[0:1] + affine[1:2]).astype(BF16)
        keep = row < counts[pl.program_id(0) * (values.shape[0] // PATCHES) + k]
        padded = jnp.concatenate([weights[here], fill], axis=0)
        grads[there] = jnp.where(keep, padded, 0.0).astype(BF16)


def prepare(counts, tokens, cotangent, gain, shift):
    rows, width = tokens.shape
    images = counts.shape[0]
    step = 2 if images % 2 == 0 else images
    source = pl.BlockSpec((step * PATCHES, width), lambda i, c: (i, 0))
    target = pl.BlockSpec((step * PADDED, width), lambda i, c: (i, 0))
    vector = pl.BlockSpec((2, width), lambda i, c: (0, 0))
    shape = (images * PADDED, width)
    return pl.pallas_call(
        prepare_kernel,
        grid_spec=pltpu.PrefetchScalarGridSpec(
            num_scalar_prefetch=1,
            grid=(images // step,),
            in_specs=[source, source, vector],
            out_specs=[target, target, target],
        ),
        out_shape=[
            jax.ShapeDtypeStruct(shape, F32),
            jax.ShapeDtypeStruct(shape, BF16),
            jax.ShapeDtypeStruct(shape, BF16),
        ],
        cost_estimate=pl.CostEstimate(
            flops=rows * width * 20, bytes_accessed=rows * width * 12, transcendentals=0
        ),
        name="prepare",
    )(counts, tokens, cotangent, jnp.stack([gain, shift]))


def attend(counts, qkv):
    images = counts.shape[0]
    rows = qkv.shape[0] // images
    group = qkv.shape[1] // 3
    heads = group // HEAD_DIM
    return pl.pallas_call(
        functools.partial(attend_kernel, group),
        grid_spec=pltpu.PrefetchScalarGridSpec(
            num_scalar_prefetch=1,
            grid=(images,),
            in_specs=[pl.BlockSpec((rows, 3 * group), lambda i, c: (i, 0))],
            out_specs=[
                pl.BlockSpec((rows, group), lambda i, c: (i, 0)),
                pl.BlockSpec((1, heads, rows, rows), lambda i, c: (i, 0, 0, 0)),
            ],
        ),
        out_shape=[
            jax.ShapeDtypeStruct((images * rows, group), BF16),
            jax.ShapeDtypeStruct((images, heads, rows, rows), BF16),
        ],
        cost_estimate=pl.CostEstimate(
            flops=images * heads * rows * rows * HEAD_DIM * 16,
            bytes_accessed=images * rows * group * 8,
            transcendentals=images * heads * rows * rows,
        ),
        name="attend",
    )(counts, qkv)


def attend_back(qkv, probs, grad_context):
    images, heads, rows, _ = probs.shape
    group = qkv.shape[1] // 3
    wide = pl.BlockSpec((rows, 3 * group), lambda i: (i, 0))
    return pl.pallas_call(
        functools.partial(attend_back_kernel, group),
        grid=(images,),
        in_specs=[
            wide,
            pl.BlockSpec((1, heads, rows, rows), lambda i: (i, 0, 0, 0)),
            pl.BlockSpec((rows, group), lambda i: (i, 0)),
        ],
        out_specs=wide,
        out_shape=jax.ShapeDtypeStruct(qkv.shape, BF16),
        cost_estimate=pl.CostEstimate(
            flops=images * heads * rows * rows * HEAD_DIM * 40,
            bytes_accessed=images * rows * group * 16,
            transcendentals=0,
        ),
        name="attend_back",
    )(qkv, probs, grad_context)


def swap(value, axis, bit):
    size = lax.axis_size(axis)
    return lax.ppermute(value, axis, [(i, i ^ bit) for i in range(size)])


def after(value, *earlier):
    return lax.optimization_barrier((value, *earlier))[0]


def on_device(
    tokens,
    res_class,
    gain_attn,
    shift_attn,
    w_qkv,
    bias_qv,
    w_out,
    bias_out,
    gain_mlp,
    shift_mlp,
    w_up,
    bias_up,
    w_down,
    bias_down,
    cotangent,
):
    rows, width = tokens.shape
    local = w_qkv.shape[2]
    images = rows // PATCHES
    place = lax.axis_index("tensor")
    ff_local = w_up.shape[1]
    group = 2 * local

    def gather(value):
        far = swap(value, "tensor", 2)
        return [value, swap(value, "tensor", 1), far, swap(far, "tensor", 1)]

    biases = gather(jnp.concatenate([bias_qv.reshape(-1), bias_up]))
    qkv_w = gather(w_qkv.reshape(width, 3 * local).T)
    out_w = gather(w_out)
    up_w = gather(w_up)
    down_w = gather(w_down)
    bq = [b[:local] for b in biases]
    bv = [b[local : 2 * local] for b in biases]
    bu = [b[2 * local :] for b in biases]

    def unpad(value):
        return value.reshape(images, PADDED, -1)[:, :PATCHES].reshape(rows, -1)

    classes = lax.dynamic_slice_in_dim(res_class, place * images, images)
    counts = jnp.where(classes == 0, PATCHES, PATCHES_LOW)
    key_valid = jnp.arange(PADDED)[None, :] < counts[:, None]
    row_valid = key_valid.reshape(-1).astype(F32)[:, None]

    inputs, in_attn, grad_low = prepare(counts, tokens, cotangent, gain_attn, shift_attn)

    zero = jnp.zeros((group,), F32)
    saved = []
    branch = bias_out
    for g in range(2):
        pair = (2 * g, 2 * g + 1)
        w_pair = jnp.concatenate([qkv_w[r].reshape(3, local, width) for r in pair], axis=1)
        w_pair = w_pair.reshape(3 * group, width)
        out_pair = jnp.concatenate([out_w[r] for r in pair], axis=0)
        bias = jnp.concatenate([bq[pair[0]], bq[pair[1]], zero, bv[pair[0]], bv[pair[1]]])
        qkv = (dot(in_attn, w_pair, NT) + bias).astype(BF16)
        context, probs = attend(counts, qkv)
        branch = branch + dot(context, out_pair, NN)
        saved.append((w_pair, out_pair, qkv, context, probs))
    hidden = inputs + branch
    normed_m, factor_m = normalize(hidden)
    in_mlp = lax.optimization_barrier((normed_m * gain_mlp + shift_mlp).astype(BF16))
    acts = []
    slopes = []
    mlp = bias_down
    for r in range(4):
        up_in = in_mlp if r == 0 else after(in_mlp, acts[r - 1])
        pre = dot(up_in, up_w[r], NN) + bu[r]
        cdf = 0.5 * (1.0 + lax.erf(pre * (2.0 ** -0.5)))
        bell = jnp.exp(-0.5 * pre * pre) * 0.3989422804014327
        acts.append((pre * cdf).astype(BF16))
        slopes.append((cdf + pre * bell).astype(BF16))
        mlp = mlp + dot(acts[r], down_w[r], NN)
    stream = (hidden + mlp) * row_valid
    block_out = unpad(stream.astype(BF16))

    def scatter(parts):
        near = parts[0] + swap(parts[1], "tensor", 1)
        far = parts[2] + swap(parts[3], "tensor", 1)
        return near + swap(far, "tensor", 2)

    dp_size = lax.axis_size("dp")
    dp_place = lax.axis_index("dp")
    bits = []
    while (1 << len(bits)) < dp_size:
        bits.append(len(bits))

    def high(bit):
        return (dp_place >> bit) % 2 == 1

    def halve(value, bit):
        rows_half = value.shape[0] // 2
        low_half, high_half = value[:rows_half], value[rows_half:]
        sent = jnp.where(high(bit), low_half, high_half)
        kept = jnp.where(high(bit), high_half, low_half)
        return kept + swap(sent, "dp", 1 << bit)

    def double(value, bit):
        other = swap(value, "dp", 1 << bit)
        return jnp.where(
            high(bit),
            jnp.concatenate([other, value], axis=0),
            jnp.concatenate([value, other], axis=0),
        )

    def finish(value, order):
        for bit in reversed(order):
            value = double(value, bit)
        return value

    y_first = bits

    grad_stream = grad_low.astype(F32)
    grad_bias_down = jnp.sum(grad_stream, axis=0)
    d_down = [dot(acts[r], grad_low, TN).astype(BF16) for r in range(4)]
    grad_low = after(grad_low, *d_down)
    down_1 = swap(d_down[1], "tensor", 1)
    down_3 = swap(d_down[3], "tensor", 1)
    down_far = swap(d_down[2] + down_3, "tensor", 2)
    d_bias_up, grads_pre, d_up = [], [], []
    grad_in_mlp = 0.0
    for r in range(4):
        back_in = grad_low if r == 0 else after(grad_low, grads_pre[r - 1])
        grad_pre = dot(back_in, down_w[r], NT) * slopes[r].astype(F32)
        d_bias_up.append(jnp.sum(grad_pre, axis=0))
        grads_pre.append(grad_pre.astype(BF16))
    up_in = after(in_mlp, grads_pre[3])
    for r in (3, 2, 1, 0):
        d_up.append(dot(up_in, grads_pre[r], TN).astype(BF16))
    d_up = d_up[::-1]
    up_1 = swap(d_up[1], "tensor", 1)
    up_3 = swap(d_up[3], "tensor", 1)
    grads_pre[0] = after(grads_pre[0], *d_up)
    for r in range(4):
        grad_in_mlp = grad_in_mlp + dot(grads_pre[r], up_w[r], NT)
    up_far = swap(d_up[2] + up_3, "tensor", 2)

    grad_gain_mlp = jnp.sum(grad_in_mlp * normed_m, axis=0)
    grad_shift_mlp = jnp.sum(grad_in_mlp, axis=0)
    grad_hidden = grad_stream + norm_back(grad_in_mlp, gain_mlp, normed_m, factor_m)
    grad_bias_out = jnp.sum(grad_hidden, axis=0)
    grad_branch = grad_hidden.astype(BF16)
    down = d_down[0] + down_1 + down_far
    for bit in y_first:
        down = halve(down, bit)
    up = d_up[0] + up_1 + up_far
    for bit in y_first:
        up = halve(up, bit)

    d_attn, d_bias_qv, lows = [None] * 4, [None] * 4, [None] * 2
    for g in (1, 0):
        w_pair, out_pair, qkv, context, probs = saved[g]
        out_grad = dot(context, grad_branch, TN).astype(BF16)
        grad_context = dot(grad_branch, out_pair, NT).astype(BF16)
        low = attend_back(qkv, probs, grad_context)
        lows[g] = low
        qkv_grad = dot(low, in_attn, TN).astype(BF16)
        grad_branch = after(grad_branch, qkv_grad)
        for k in range(2):
            r = 2 * g + k
            blocks = [qkv_grad[(2 * i + k) * local : (2 * i + k + 1) * local] for i in range(3)]
            d_attn[r] = jnp.concatenate(blocks + [out_grad[k * local : (k + 1) * local]], axis=0)
    far_attn = d_attn[2] + swap(d_attn[3], "tensor", 1)
    got_far = swap(far_attn, "tensor", 2)
    lows = lax.optimization_barrier((lows[0], lows[1], qkv_grad))[:2]
    grad_in_attn = dot(lows[0], saved[0][0], NN)
    grad_in_attn = grad_in_attn + dot(lows[1], saved[1][0], NN)
    own_down = finish(down, y_first)
    own_up = finish(up, y_first)
    attn = d_attn[0] + swap(d_attn[1], "tensor", 1) + got_far
    half = attn.shape[0] // 2
    pieces = []
    for piece, order in ((attn[:half], y_first), (attn[half:], y_first)):
        for bit in order:
            piece = halve(piece, bit)
        pieces.append(finish(piece, order))
    own_attn = jnp.concatenate(pieces, axis=0).astype(F32)
    own_qkv = own_attn[: 3 * local].T.reshape(width, 3, local)
    own_out = own_attn[3 * local :]
    late = lax.optimization_barrier((inputs, grad_in_attn, lows[0], lows[1], attn))
    inputs, grad_in_attn = late[:2]
    for g in range(2):
        bias_sum = jnp.sum(late[2 + g].astype(F32), axis=0).reshape(3, 2, local)
        for k in range(2):
            d_bias_qv[2 * g + k] = jnp.concatenate([bias_sum[0, k], bias_sum[2, k]])
    normed_a, factor_a = normalize(inputs)
    grad_gain_attn = jnp.sum(grad_in_attn * normed_a, axis=0)
    grad_shift_attn = jnp.sum(grad_in_attn, axis=0)
    grad_tokens = grad_hidden + norm_back(grad_in_attn, gain_attn, normed_a, factor_a)
    grad_tokens = unpad(grad_tokens)
    totals = jnp.stack(
        [
            jnp.sum(stream * stream),
            jnp.sum(branch * branch * row_valid),
            jnp.sum(mlp * mlp * row_valid),
            jnp.sum(row_valid),
        ]
    )
    shared = jnp.concatenate(
        [
            grad_gain_attn,
            grad_shift_attn,
            grad_bias_out,
            grad_gain_mlp,
            grad_shift_mlp,
            grad_bias_down,
            totals,
        ]
    )
    shared = after(shared, attn)
    shared = shared + swap(shared, "tensor", 1)
    shared = shared + swap(shared, "tensor", 2)
    biases = scatter([jnp.concatenate([d_bias_qv[r], d_bias_up[r]]) for r in range(4)])
    small = jnp.concatenate([biases, shared])
    for bit in bits:
        small = small + swap(small, "dp", 1 << bit)
    wide = 2 * local + ff_local
    got = [small[wide + i * width : wide + (i + 1) * width] for i in range(6)]
    sums = small[wide + 6 * width :]
    rms = jnp.sqrt(sums[:3] / (sums[3] * width))
    return (
        block_out,
        grad_tokens,
        got[0],
        got[1],
        own_qkv,
        small[: 2 * local].reshape(2, local),
        own_out,
        got[2],
        got[3],
        got[4],
        own_up.astype(F32),
        small[2 * local : wide],
        own_down.astype(F32),
        got[5],
        rms,
    )


def solution(mesh):
    row = P(("dp", "tensor"), None)
    in_specs = (
        row, P("dp"), P(), P(), P(None, None, "tensor"), P(None, "tensor"), P("tensor", None),
        P(), P(), P(), P(None, "tensor"), P("tensor"), P("tensor", None), P(), row,
    )
    out_specs = (
        row, row, P(), P(), P(None, None, "tensor"), P(None, "tensor"), P("tensor", None),
        P(), P(), P(), P(None, "tensor"), P("tensor"), P("tensor", None), P(), P(),
    )
    return jax.shard_map(
        on_device, mesh=mesh, in_specs=in_specs, out_specs=out_specs, check_vma=False
    )
```

```python
import functools

import jax
import jax.numpy as jnp
from jax import lax
from jax.experimental import pallas as pl
from jax.experimental.pallas import tpu as pltpu
from jax.sharding import PartitionSpec as P


HEAD_DIM = 64
PATCHES = 196
PATCHES_LOW = 144
PADDED = 208
LANES = 128
EPS = 1e-06
F32 = jnp.float32
BF16 = jnp.bfloat16


def normalize(values):
    mean = jnp.mean(values, axis=-1, keepdims=True)
    centred = values - mean
    factor = lax.rsqrt(jnp.mean(centred * centred, axis=-1, keepdims=True) + EPS)
    return (centred * factor, factor)


def norm_back(grad_out, gain, normed, factor):
    scaled = grad_out * gain
    return factor * (
        scaled
        - jnp.mean(scaled, axis=-1, keepdims=True)
        - normed * jnp.mean(scaled * normed, axis=-1, keepdims=True)
    )


def dot(a, b, dims):
    return lax.dot_general(a, b, (dims, ((), ())), preferred_element_type=F32)


NN = ((1,), (0,))
NT = ((1,), (1,))
TN = ((0,), (0,))


def head_masks(factor):
    lane = lax.broadcasted_iota(jnp.int32, (1, LANES), 1)
    first = jnp.where(lane < HEAD_DIM, factor, 0.0)
    return first.astype(BF16), (factor - first).astype(BF16)


def attend_kernel(group, counts, qkv, context, probs):
    rows = qkv.shape[0]
    valid = counts[pl.program_id(0)]
    keep = lax.broadcasted_iota(jnp.int32, (rows, rows), 1) < valid
    ones = head_masks(1.0)
    scaled = head_masks(HEAD_DIM ** (-0.5))
    for j in range(group // LANES):
        at = j * LANES
        query = qkv[:, at : at + LANES]
        key = qkv[:, group + at : group + at + LANES]
        value = qkv[:, 2 * group + at : 2 * group + at + LANES]
        total = None
        for h in range(2):
            scores = dot(query * scaled[h], key, NT)
            scores = jnp.where(keep, scores, -1e30)
            top = jnp.max(scores, axis=-1, keepdims=True)
            raised = jnp.exp(scores - top)
            low = (raised * (1.0 / jnp.sum(raised, axis=-1, keepdims=True))).astype(BF16)
            probs[0, 2 * j + h] = low
            part = dot(low, value * ones[h], NN)
            total = part if total is None else total + part
        context[:, at : at + LANES] = total.astype(BF16)


def attend_back_kernel(group, qkv, probs, grad_context, grads):
    ones = head_masks(1.0)
    scaled = head_masks(HEAD_DIM ** (-0.5))
    for j in range(group // LANES):
        at = j * LANES
        query = qkv[:, at : at + LANES]
        key = qkv[:, group + at : group + at + LANES]
        value = qkv[:, 2 * group + at : 2 * group + at + LANES]
        grad = grad_context[:, at : at + LANES]
        sums = None
        for h in range(2):
            own = grad * ones[h]
            low = probs[0, 2 * j + h]
            wide = low.astype(F32)
            grad_probs = dot(own, value, NT)
            row_dot = jnp.sum(wide * grad_probs, axis=-1, keepdims=True)
            grad_scores = (wide * (grad_probs - row_dot)).astype(BF16)
            parts = (
                dot(grad_scores, key * scaled[h], NN),
                dot(grad_scores, query * scaled[h], TN),
                dot(low, own, TN),
            )
            sums = parts if sums is None else [a + b for a, b in zip(sums, parts)]
        for i in range(3):
            grads[:, i * group + at : i * group + at + LANES] = sums[i].astype(BF16)


def prepare_kernel(counts, tokens, cotangent, affine, inputs, in_attn, grads):
    values = tokens[...].astype(F32)
    weights = cotangent[...].astype(F32)
    width = values.shape[1]
    fill = jnp.zeros((PADDED - PATCHES, width), F32)
    row = lax.broadcasted_iota(jnp.int32, (PADDED, 1), 0)
    for k in range(values.shape[0] // PATCHES):
        here = slice(k * PATCHES, (k + 1) * PATCHES)
        there = slice(k * PADDED, (k + 1) * PADDED)
        padded = jnp.concatenate([values[here], fill], axis=0)
        inputs[there] = padded
        in_attn[there] = (normalize(padded)[0] * affine[0:1] + affine[1:2]).astype(BF16)
        keep = row < counts[pl.program_id(0) * (values.shape[0] // PATCHES) + k]
        padded = jnp.concatenate([weights[here], fill], axis=0)
        grads[there] = jnp.where(keep, padded, 0.0).astype(BF16)


def prepare(counts, tokens, cotangent, gain, shift):
    rows, width = tokens.shape
    images = counts.shape[0]
    step = 2 if images % 2 == 0 else images
    source = pl.BlockSpec((step * PATCHES, width), lambda i, c: (i, 0))
    target = pl.BlockSpec((step * PADDED, width), lambda i, c: (i, 0))
    vector = pl.BlockSpec((2, width), lambda i, c: (0, 0))
    shape = (images * PADDED, width)
    return pl.pallas_call(
        prepare_kernel,
        grid_spec=pltpu.PrefetchScalarGridSpec(
            num_scalar_prefetch=1,
            grid=(images // step,),
            in_specs=[source, source, vector],
            out_specs=[target, target, target],
        ),
        out_shape=[
            jax.ShapeDtypeStruct(shape, F32),
            jax.ShapeDtypeStruct(shape, BF16),
            jax.ShapeDtypeStruct(shape, BF16),
        ],
        cost_estimate=pl.CostEstimate(
            flops=rows * width * 20, bytes_accessed=rows * width * 12, transcendentals=0
        ),
        name="prepare",
    )(counts, tokens, cotangent, jnp.stack([gain, shift]))


def attend(counts, qkv):
    images = counts.shape[0]
    rows = qkv.shape[0] // images
    group = qkv.shape[1] // 3
    heads = group // HEAD_DIM
    return pl.pallas_call(
        functools.partial(attend_kernel, group),
        grid_spec=pltpu.PrefetchScalarGridSpec(
            num_scalar_prefetch=1,
            grid=(images,),
            in_specs=[pl.BlockSpec((rows, 3 * group), lambda i, c: (i, 0))],
            out_specs=[
                pl.BlockSpec((rows, group), lambda i, c: (i, 0)),
                pl.BlockSpec((1, heads, rows, rows), lambda i, c: (i, 0, 0, 0)),
            ],
        ),
        out_shape=[
            jax.ShapeDtypeStruct((images * rows, group), BF16),
            jax.ShapeDtypeStruct((images, heads, rows, rows), BF16),
        ],
        cost_estimate=pl.CostEstimate(
            flops=images * heads * rows * rows * HEAD_DIM * 16,
            bytes_accessed=images * rows * group * 8,
            transcendentals=images * heads * rows * rows,
        ),
        name="attend",
    )(counts, qkv)


def attend_back(qkv, probs, grad_context):
    images, heads, rows, _ = probs.shape
    group = qkv.shape[1] // 3
    wide = pl.BlockSpec((rows, 3 * group), lambda i: (i, 0))
    return pl.pallas_call(
        functools.partial(attend_back_kernel, group),
        grid=(images,),
        in_specs=[
            wide,
            pl.BlockSpec((1, heads, rows, rows), lambda i: (i, 0, 0, 0)),
            pl.BlockSpec((rows, group), lambda i: (i, 0)),
        ],
        out_specs=wide,
        out_shape=jax.ShapeDtypeStruct(qkv.shape, BF16),
        cost_estimate=pl.CostEstimate(
            flops=images * heads * rows * rows * HEAD_DIM * 40,
            bytes_accessed=images * rows * group * 16,
            transcendentals=0,
        ),
        name="attend_back",
    )(qkv, probs, grad_context)


def swap(value, axis, bit):
    size = lax.axis_size(axis)
    return lax.ppermute(value, axis, [(i, i ^ bit) for i in range(size)])


def after(value, *earlier):
    return lax.optimization_barrier((value, *earlier))[0]


def on_device(
    tokens,
    res_class,
    gain_attn,
    shift_attn,
    w_qkv,
    bias_qv,
    w_out,
    bias_out,
    gain_mlp,
    shift_mlp,
    w_up,
    bias_up,
    w_down,
    bias_down,
    cotangent,
):
    rows, width = tokens.shape
    local = w_qkv.shape[2]
    images = rows // PATCHES
    place = lax.axis_index("tensor")
    ff_local = w_up.shape[1]
    group = 2 * local

    def gather(value):
        far = swap(value, "tensor", 2)
        return [value, swap(value, "tensor", 1), far, swap(far, "tensor", 1)]

    biases = gather(jnp.concatenate([bias_qv.reshape(-1), bias_up]))
    qkv_w = gather(w_qkv.reshape(width, 3 * local).T)
    out_w = gather(w_out)
    up_w = gather(w_up)
    down_w = gather(w_down)
    bq = [b[:local] for b in biases]
    bv = [b[local : 2 * local] for b in biases]
    bu = [b[2 * local :] for b in biases]

    def unpad(value):
        return value.reshape(images, PADDED, -1)[:, :PATCHES].reshape(rows, -1)

    classes = lax.dynamic_slice_in_dim(res_class, place * images, images)
    counts = jnp.where(classes == 0, PATCHES, PATCHES_LOW)
    key_valid = jnp.arange(PADDED)[None, :] < counts[:, None]
    row_valid = key_valid.reshape(-1).astype(F32)[:, None]

    inputs, in_attn, grad_low = prepare(counts, tokens, cotangent, gain_attn, shift_attn)

    zero = jnp.zeros((group,), F32)
    saved = []
    branch = bias_out
    for g in range(2):
        pair = (2 * g, 2 * g + 1)
        w_pair = jnp.concatenate([qkv_w[r].reshape(3, local, width) for r in pair], axis=1)
        w_pair = w_pair.reshape(3 * group, width)
        out_pair = jnp.concatenate([out_w[r] for r in pair], axis=0)
        bias = jnp.concatenate([bq[pair[0]], bq[pair[1]], zero, bv[pair[0]], bv[pair[1]]])
        qkv = (dot(in_attn, w_pair, NT) + bias).astype(BF16)
        context, probs = attend(counts, qkv)
        branch = branch + dot(context, out_pair, NN)
        saved.append((w_pair, out_pair, qkv, context, probs))
    hidden = inputs + branch
    normed_m, factor_m = normalize(hidden)
    in_mlp = lax.optimization_barrier((normed_m * gain_mlp + shift_mlp).astype(BF16))
    acts = []
    slopes = []
    mlp = bias_down
    for r in range(4):
        up_in = in_mlp if r == 0 else after(in_mlp, acts[r - 1])
        pre = dot(up_in, up_w[r], NN) + bu[r]
        cdf = 0.5 * (1.0 + lax.erf(pre * (2.0 ** -0.5)))
        bell = jnp.exp(-0.5 * pre * pre) * 0.3989422804014327
        acts.append((pre * cdf).astype(BF16))
        slopes.append((cdf + pre * bell).astype(BF16))
        mlp = mlp + dot(acts[r], down_w[r], NN)
    stream = (hidden + mlp) * row_valid
    stream_low = stream.astype(BF16)

    def scatter(parts):
        near = parts[0] + swap(parts[1], "tensor", 1)
        far = parts[2] + swap(parts[3], "tensor", 1)
        return near + swap(far, "tensor", 2)

    dp_size = lax.axis_size("dp")
    dp_place = lax.axis_index("dp")
    bits = []
    while (1 << len(bits)) < dp_size:
        bits.append(len(bits))

    def high(bit):
        return (dp_place >> bit) % 2 == 1

    def halve(value, bit):
        rows_half = value.shape[0] // 2
        low_half, high_half = value[:rows_half], value[rows_half:]
        sent = jnp.where(high(bit), low_half, high_half)
        kept = jnp.where(high(bit), high_half, low_half)
        return kept + swap(sent, "dp", 1 << bit)

    def double(value, bit):
        other = swap(value, "dp", 1 << bit)
        return jnp.where(
            high(bit),
            jnp.concatenate([other, value], axis=0),
            jnp.concatenate([value, other], axis=0),
        )

    def finish(value, order):
        for bit in reversed(order):
            value = double(value, bit)
        return value

    y_first = bits

    grad_stream = grad_low.astype(F32)
    grad_bias_down = jnp.sum(grad_stream, axis=0)
    d_down = [dot(acts[r], grad_low, TN).astype(BF16) for r in range(4)]
    grad_low = after(grad_low, *d_down)
    down_1 = swap(d_down[1], "tensor", 1)
    down_3 = swap(d_down[3], "tensor", 1)
    down_far = swap(d_down[2] + down_3, "tensor", 2)
    d_bias_up, grads_pre, d_up = [], [], []
    grad_in_mlp = 0.0
    for r in range(4):
        back_in = grad_low if r == 0 else after(grad_low, grads_pre[r - 1])
        grad_pre = dot(back_in, down_w[r], NT) * slopes[r].astype(F32)
        d_bias_up.append(jnp.sum(grad_pre, axis=0))
        grads_pre.append(grad_pre.astype(BF16))
    up_in = after(in_mlp, grads_pre[3])
    for r in (3, 2, 1, 0):
        d_up.append(dot(up_in, grads_pre[r], TN).astype(BF16))
    d_up = d_up[::-1]
    up_1 = swap(d_up[1], "tensor", 1)
    up_3 = swap(d_up[3], "tensor", 1)
    grads_pre[0] = after(grads_pre[0], *d_up)
    for r in range(4):
        grad_in_mlp = grad_in_mlp + dot(grads_pre[r], up_w[r], NT)
    up_far = swap(d_up[2] + up_3, "tensor", 2)

    grad_gain_mlp = jnp.sum(grad_in_mlp * normed_m, axis=0)
    grad_shift_mlp = jnp.sum(grad_in_mlp, axis=0)
    grad_hidden = grad_stream + norm_back(grad_in_mlp, gain_mlp, normed_m, factor_m)
    grad_bias_out = jnp.sum(grad_hidden, axis=0)
    grad_branch = grad_hidden.astype(BF16)
    down = d_down[0] + down_1 + down_far
    for bit in y_first:
        down = halve(down, bit)
    up = d_up[0] + up_1 + up_far
    for bit in y_first:
        up = halve(up, bit)

    d_attn, d_bias_qv, lows = [None] * 4, [None] * 4, [None] * 2
    for g in (1, 0):
        w_pair, out_pair, qkv, context, probs = saved[g]
        out_grad = dot(context, grad_branch, TN).astype(BF16)
        grad_context = dot(grad_branch, out_pair, NT).astype(BF16)
        low = attend_back(qkv, probs, grad_context)
        lows[g] = low
        qkv_grad = dot(low, in_attn, TN).astype(BF16)
        grad_branch = after(grad_branch, qkv_grad)
        for k in range(2):
            r = 2 * g + k
            blocks = [qkv_grad[(2 * i + k) * local : (2 * i + k + 1) * local] for i in range(3)]
            d_attn[r] = jnp.concatenate(blocks + [out_grad[k * local : (k + 1) * local]], axis=0)
    far_attn = d_attn[2] + swap(d_attn[3], "tensor", 1)
    got_far = swap(far_attn, "tensor", 2)
    lows = lax.optimization_barrier((lows[0], lows[1], qkv_grad))[:2]
    grad_in_attn = dot(lows[0], saved[0][0], NN)
    grad_in_attn = grad_in_attn + dot(lows[1], saved[1][0], NN)
    own_down = finish(down, y_first)
    own_up = finish(up, y_first)
    attn = d_attn[0] + swap(d_attn[1], "tensor", 1) + got_far
    half = attn.shape[0] // 2
    pieces = []
    for piece, order in ((attn[:half], y_first), (attn[half:], y_first)):
        for bit in order:
            piece = halve(piece, bit)
        pieces.append(finish(piece, order))
    own_attn = jnp.concatenate(pieces, axis=0).astype(F32)
    own_qkv = own_attn[: 3 * local].T.reshape(width, 3, local)
    own_out = own_attn[3 * local :]
    late = lax.optimization_barrier((inputs, grad_in_attn, lows[0], lows[1], stream_low, attn))
    block_out = unpad(late[4])
    inputs, grad_in_attn = late[:2]
    for g in range(2):
        bias_sum = jnp.sum(late[2 + g].astype(F32), axis=0).reshape(3, 2, local)
        for k in range(2):
            d_bias_qv[2 * g + k] = jnp.concatenate([bias_sum[0, k], bias_sum[2, k]])
    normed_a, factor_a = normalize(inputs)
    grad_gain_attn = jnp.sum(grad_in_attn * normed_a, axis=0)
    grad_shift_attn = jnp.sum(grad_in_attn, axis=0)
    grad_tokens = grad_hidden + norm_back(grad_in_attn, gain_attn, normed_a, factor_a)
    grad_tokens = unpad(grad_tokens)
    totals = jnp.stack(
        [
            jnp.sum(stream * stream),
            jnp.sum(branch * branch * row_valid),
            jnp.sum(mlp * mlp * row_valid),
            jnp.sum(row_valid),
        ]
    )
    shared = jnp.concatenate(
        [
            grad_gain_attn,
            grad_shift_attn,
            grad_bias_out,
            grad_gain_mlp,
            grad_shift_mlp,
            grad_bias_down,
            totals,
        ]
    )
    shared = after(shared, attn)
    shared = shared + swap(shared, "tensor", 1)
    shared = shared + swap(shared, "tensor", 2)
    biases = scatter([jnp.concatenate([d_bias_qv[r], d_bias_up[r]]) for r in range(4)])
    small = jnp.concatenate([biases, shared])
    for bit in bits:
        small = small + swap(small, "dp", 1 << bit)
    wide = 2 * local + ff_local
    got = [small[wide + i * width : wide + (i + 1) * width] for i in range(6)]
    sums = small[wide + 6 * width :]
    rms = jnp.sqrt(sums[:3] / (sums[3] * width))
    return (
        block_out,
        grad_tokens,
        got[0],
        got[1],
        own_qkv,
        small[: 2 * local].reshape(2, local),
        own_out,
        got[2],
        got[3],
        got[4],
        own_up.astype(F32),
        small[2 * local : wide],
        own_down.astype(F32),
        got[5],
        rms,
    )


def solution(mesh):
    row = P(("dp", "tensor"), None)
    in_specs = (
        row, P("dp"), P(), P(), P(None, None, "tensor"), P(None, "tensor"), P("tensor", None),
        P(), P(), P(), P(None, "tensor"), P("tensor"), P("tensor", None), P(), row,
    )
    out_specs = (
        row, row, P(), P(), P(None, None, "tensor"), P(None, "tensor"), P("tensor", None),
        P(), P(), P(), P(None, "tensor"), P("tensor"), P("tensor", None), P(), P(),
    )
    return jax.shard_map(
        on_device, mesh=mesh, in_specs=in_specs, out_specs=out_specs, check_vma=False
    )
```
